32 devices in a mesh: replica: 4 (over y, x), fsdp: 8 (over z, core).
Axes of the slice: x: 2, y: 2, z: 4, core: 2. Of those that a mesh axis runs over, the one named last changes fastest.
Arguments:
- base_weights: float32 [8192, 1024], P('fsdp'), may hold values from -5 to 5, as said below
- inner_weights: bfloat16 [4, 8192, 1024], P('replica', 'fsdp'), may hold values from -12 to 12, as said below
- momentum: float32 [8192, 1024], P(('fsdp', 'replica')), may hold values from -1 to 1
Outputs:
- new_base: float32 [8192, 1024], P('fsdp')
- new_momentum: float32 [8192, 1024], P(('fsdp', 'replica'))
- new_inner: bfloat16 [4, 8192, 1024], P('replica', 'fsdp')
The draws below stay inside these ranges and needn't reach their ends.
Inputs may be any that keep to these rules, and one draw needn't show every extreme that they name: `base_weights`: the shared outer weights, multiples of 2 ** -16. `inner_weights`: each replica's weights after its inner steps, multiples of 2 ** -16.
All inputs are finite; a program needn't handle non-finite values.
Results may differ from the reference program's by a relative error of at most 0.0015.
Values may be sent and summed in bfloat16 or wider, within the bound.
A program may use at most 64 MiB of HBM per device.

```python
import jax
import jax.numpy as jnp
from jax import lax

D = 8192
KVW = 1024
BLOCK = 128
REPLICAS = 4


grid_step = 65536.0


def draw_common(key):
    folded = jax.random.fold_in(key, 11)
    base_key = jax.random.fold_in(folded, 0)
    column_key = jax.random.fold_in(folded, 1)
    own_key = jax.random.fold_in(folded, 2)
    row_key = jax.random.fold_in(folded, 4)
    base_values = jnp.clip(jax.random.normal(base_key, (D, KVW), jnp.float32), -5.0, 5.0)
    base_values = jnp.floor(base_values * grid_step + 0.5) / grid_step
    columns = jnp.exp(jax.random.uniform(column_key, (KVW,), jnp.float32, 0.0, jnp.log(10.0)))
    row_scale = 0.1 * jnp.exp(jax.random.uniform(row_key, (D,), jnp.float32, -jnp.log(1000.0), 0.0))
    copies = jnp.exp(jnp.log(3.0) * jnp.arange(REPLICAS, dtype=jnp.float32) / (REPLICAS - 1))
    own_noise = jax.random.uniform(own_key, (REPLICAS, D, KVW), jnp.float32, -1.0, 1.0)
    perturb = own_noise
    deltas = perturb * row_scale[None, :, None] * columns[None, None, :] * copies[:, None, None]
    inner_values = base_values[None] - deltas
    inner_values = jnp.floor(inner_values * grid_step + 0.5) / grid_step
    return (base_values, inner_values)


def draw_base_weights(key, part):
    base_values, inner_values = draw_common(key)
    return base_values.astype(jnp.float32)


def draw_inner_weights(key, part):
    base_values, inner_values = draw_common(key)
    return inner_values.astype(jnp.bfloat16)


def levels(key, dims, pieces, low, top_value):
    def one(axis_at, parts):
        draws = jax.random.uniform(jax.random.fold_in(jax.random.fold_in(key, 6), axis_at), (parts,), jnp.float32, low / len(pieces), top_value / len(pieces))
        return jnp.repeat(jnp.exp(draws), dims[axis_at] // parts).reshape((-1,) + (1,) * (len(dims) - axis_at - 1))

    gain = one(*pieces[0])
    for cut in pieces[1:]:
        gain = gain * one(*cut)
    return gain


def scatter_about(key, dims, spread, most, pieces=(), held_as=jnp.bfloat16):
    factor_of = levels(key, dims, pieces, -0.22, 0.18) if pieces else 1.0
    array = jax.random.normal(key, dims, jnp.float32) * spread * factor_of
    return jnp.minimum(jnp.maximum(array, -most), most).astype(held_as)


def setup_inputs(seed: int = 0) -> dict:
    key_of = jax.random.split(jax.random.key(seed), 4)
    return {
        "base_weights": draw_base_weights(jax.random.fold_in(key_of[3], 71), 0),
        "inner_weights": draw_inner_weights(jax.random.fold_in(key_of[3], 71), 0),
        "momentum": scatter_about(key_of[2], (D, KVW), 0.2, 1.0, ((0, 32),), jnp.float32),
    }


code_limit = 448.0
outer_rate = 0.7
outer_momentum = 0.9
blend_share = 0.5
clip_rms = 0.02
epsilon = 1e-06
smallest_normal = 0.015625

def power_two(exponent):
    unit_ones = jnp.ones_like(exponent)
    upward = jnp.left_shift(unit_ones, jnp.maximum(exponent, 0)).astype(jnp.float32)
    downward = jnp.left_shift(unit_ones, jnp.maximum(-exponent, 0)).astype(jnp.float32)
    return upward / downward

def exponent_above(target):
    estimate = jnp.ceil(jnp.log2(target)).astype(jnp.int32)
    estimate = jnp.where(target <= power_two(estimate - 1), estimate - 1, estimate)
    return jnp.where(target > power_two(estimate), estimate + 1, estimate)

def exponent_below(target):
    estimate = jnp.floor(jnp.log2(target)).astype(jnp.int32)
    estimate = jnp.where(target >= power_two(estimate + 1), estimate + 1, estimate)
    return jnp.where(target < power_two(estimate), estimate - 1, estimate)

def encode(deltas):
    shaped = deltas.reshape(deltas.shape[0], deltas.shape[1] // BLOCK, BLOCK)
    block_peaks = lax.optimization_barrier(jnp.max(jnp.abs(shaped), axis=2))
    scales = power_two(exponent_above((block_peaks + epsilon) / code_limit))
    code_units = shaped / scales[:, :, None]
    magnitude = jnp.abs(code_units)
    quantum = power_two(exponent_below(jnp.maximum(magnitude, smallest_normal)) - 3)
    steps_count = jnp.floor(magnitude / quantum + 0.5)
    code_values = (jnp.where(code_units < 0, -steps_count, steps_count) * quantum).astype(jnp.bfloat16)
    return (code_values, scales)

def reference(base_weights, inner_weights, momentum):

    def add_replica(summed, replica_copy):
        deltas = base_weights - replica_copy.astype(jnp.float32)
        code_values, scales = encode(deltas)
        decoded = code_values.astype(jnp.float32) * scales[:, :, None]
        return (summed + decoded.reshape(deltas.shape), None)
    summed, unused = lax.scan(add_replica, jnp.zeros(base_weights.shape, jnp.float32), inner_weights)
    outer_grad = summed / REPLICAS
    grad_sq = jnp.sum(outer_grad * outer_grad)
    clip_factor = jnp.minimum(1.0, clip_rms / jnp.sqrt(grad_sq / (D * KVW) + epsilon))
    step_term = clip_factor * outer_grad
    new_momentum = outer_momentum * momentum + step_term
    new_base = base_weights - outer_rate * (step_term + outer_momentum * new_momentum)

    def blend_one(replica_copy):
        blended = blend_share * replica_copy.astype(jnp.float32) + (1.0 - blend_share) * new_base
        return blended.astype(jnp.bfloat16)
    new_inner = lax.map(blend_one, inner_weights)
    return (new_base, new_momentum, new_inner)
```

```python
import functools

import jax
import jax.numpy as jnp
from jax import lax
from jax.experimental import pallas as pl
from jax.experimental.pallas import tpu as pltpu
from jax.sharding import PartitionSpec as P

BLOCK = 128
HALF_GROUPS = 4
EARLY_GROUPS = 2
ENCODE_ROWS = 256
PLAIN_ROWS = 128

code_limit = 448.0
outer_rate = 0.7
outer_momentum = 0.9
blend_share = 0.5
clip_rms = 0.02
epsilon = 1e-06

MESH = pl.DeviceIdType.MESH


def decoded_deltas(deltas):
    peaks = jnp.max(jnp.abs(deltas), axis=1, keepdims=True) + epsilon
    rough = peaks * (1.0 / code_limit)
    wide = rough * (2.0**23 + 1.0)
    power = wide - (wide - rough)
    scales = jnp.where(power * code_limit < peaks, power + power, power)
    nudged = deltas * (1.0 + 2.0**-23)
    wide_deltas = nudged * (2.0**20 + 1.0)
    four_bits = wide_deltas - (wide_deltas - nudged)
    shift = scales * (1.5 * 2.0**14)
    fixed_step = (nudged + shift) - shift
    return jnp.where(jnp.abs(deltas) < scales * 2.0**-6, fixed_step, four_bits)


def arrived(blocks, sem):
    pltpu.make_async_copy(blocks, blocks, sem).wait()


def grid_sides(replicas):
    side = 1 << (replicas.bit_length() // 2)
    while replicas % side:
        side -= 1
    return side, replicas // side


def kernel(
    dims,
    base_hbm, inner_hbm, momentum_hbm,
    new_base, new_momentum, new_inner,
    base_v, inner_v, momentum_v, dec, first, second, grad, update, early,
    square_mine, square_near, square_row, square_far,
    load_sems, send_sems, recv_sems, early_sems, square_sems, entry_sems,
):
    replicas, shards_count, rows, columns, groups, total = dims
    width = columns // groups
    span_x, span_y = grid_sides(replicas)
    tile = min(PLAIN_ROWS, rows)
    encode_tile = min(ENCODE_ROWS, rows)
    me = lax.axis_index("replica")
    row_me = lax.axis_index("fsdp")
    me_x, me_y = lax.rem(me, span_x), me // span_x

    def spans(g):
        return (span_x, span_y) if g % 2 == 0 else (span_y, span_x)

    def owner(g, dp, dq):
        dx, dy = (dp, dq) if g % 2 == 0 else (dq, dp)
        return lax.rem(me_y + dy, span_y) * span_x + lax.rem(me_x + dx, span_x)

    def near(step):
        return lax.rem(me + step, replicas)

    def far(step):
        return lax.rem(row_me + step, shards_count)

    def row_start(index):
        return pl.multiple_of(index * rows, rows)

    barrier = pltpu.get_barrier_semaphore()
    for step in range(1, replicas):
        pl.semaphore_signal(barrier, inc=1, device_id={"replica": near(step)}, device_id_type=MESH)
    for step in range(1, shards_count):
        pl.semaphore_signal(barrier, inc=1, device_id={"fsdp": far(step)}, device_id_type=MESH)

    load_order = [(dx, dy) for dy in reversed(range(span_y)) for dx in reversed(range(span_x))]
    loads = []
    for at, (dx, dy) in enumerate(load_order):
        here = pl.ds(row_start(owner(0, dx, dy)), rows)
        pair = (
            pltpu.make_async_copy(base_hbm.at[here], base_v.at[here], load_sems.at[at, 0]),
            pltpu.make_async_copy(inner_hbm.at[0, here], inner_v.at[here], load_sems.at[at, 1]),
        )
        for copy in pair:
            copy.start()
        loads.append(pair)
    momentum_load = pltpu.make_async_copy(momentum_hbm, momentum_v, load_sems.at[replicas, 0])
    momentum_load.start()

    def encode(g, dp, dq):
        slot = dp * spans(g)[1] + dq
        start = row_start(owner(g, dp, dq))

        @pl.loop(0, rows // encode_tile)
        def _(t):
            at = pl.ds(pl.multiple_of(start + t * encode_tile, encode_tile), encode_tile)
            to = pl.ds(pl.multiple_of(t * encode_tile, encode_tile), encode_tile)
            for c in range(0, width, BLOCK):
                cols = pl.ds(g * width + c, BLOCK)
                deltas = base_v[at, cols] - inner_v[at, cols].astype(jnp.float32)
                dec[g, slot, to, pl.ds(c, BLOCK)] = decoded_deltas(deltas).astype(jnp.bfloat16)

    def copy_one(g, dp, dq):
        slot = dp * spans(g)[1] + dq
        return pltpu.make_async_remote_copy(
            src_ref=dec.at[g, slot], dst_ref=first.at[g, slot],
            send_sem=send_sems.at[0], recv_sem=recv_sems.at[g, slot - 1],
            device_id={"replica": owner(g, dp, 0)}, device_id_type=MESH,
        )

    def copy_two(g, dq):
        return pltpu.make_async_remote_copy(
            src_ref=dec.at[g, dq], dst_ref=second.at[g, dq],
            send_sem=send_sems.at[0], recv_sem=recv_sems.at[g, dq - 1],
            device_id={"replica": owner(g, 0, dq)}, device_id_type=MESH,
        )

    def arrival(g, dp, dq, source):
        np, nq = spans(g)
        return ((np - dp) % np) * nq + (source if dp else (nq - dq) % nq)

    def copy_all(g, dp, dq, source):
        slot = arrival(g, dp, dq, source)
        return pltpu.make_async_remote_copy(
            src_ref=update.at[g, source if dp else 0], dst_ref=update.at[g, slot],
            send_sem=send_sems.at[1], recv_sem=recv_sems.at[g, slot - 1],
            device_id={"replica": owner(g, dp, dq)}, device_id_type=MESH,
        )

    def copy_early(g, part, dp, dq, source):
        slot = arrival(g, dp, dq, source)
        return pltpu.make_async_remote_copy(
            src_ref=early.at[g, part, source if dp else 0], dst_ref=early.at[g, part, slot],
            send_sem=send_sems.at[2], recv_sem=early_sems.at[g, part, slot - 1],
            device_id={"replica": owner(g, dp, dq)}, device_id_type=MESH,
        )

    waited = set()

    def await_load(g, dp, dq):
        key = (dp, dq) if g % 2 == 0 else (dq, dp)
        if key not in waited:
            waited.add(key)
            for copy in loads[load_order.index(key)]:
                copy.wait()

    greeted = False
    most = max(span_x, span_y)
    for dq in reversed(range(most)):
        for dp in reversed(range(1, most)):
            for g in range(groups):
                np, nq = spans(g)
                if dp < np and dq < nq:
                    await_load(g, dp, dq)
                    encode(g, dp, dq)
                    if not greeted:
                        pl.semaphore_wait(barrier, replicas - 1 + shards_count - 1)
                        greeted = True
                    copy_one(g, dp, dq).start()
    for dq in reversed(range(most)):
        for g in range(groups):
            if dq < spans(g)[1]:
                await_load(g, 0, dq)
                encode(g, 0, dq)

    for dq in reversed(range(most)):
        for g in range(groups):
            np, nq = spans(g)
            if dq >= nq:
                continue
            for dp in range(1, np):
                copy_one(g, dp, dq).wait_recv()

            @pl.loop(0, rows // tile)
            def _(t):
                at = pl.ds(pl.multiple_of(t * tile, tile), tile)
                summed = dec[g, dq, at].astype(jnp.float32)
                for dp in range(1, np):
                    summed += first[g, dp * nq + dq, at].astype(jnp.float32)
                if dq:
                    dec[g, dq, at] = summed.astype(jnp.bfloat16)
                else:
                    grad[at, pl.ds(g * width, width)] = summed

            if dq:
                copy_two(g, dq).start()

    def add_group(g, squares):
        nq = spans(g)[1]
        for dq in range(1, nq):
            copy_two(g, dq).wait_recv()

        def add(t, squares):
            at = pl.ds(pl.multiple_of(t * tile, tile), tile)
            for c in range(0, width, BLOCK):
                cols = pl.ds(g * width + c, BLOCK)
                summed = grad[at, cols]
                for dq in range(1, nq):
                    summed += second[g, dq, at, pl.ds(c, BLOCK)].astype(jnp.float32)
                outer = summed * (1.0 / replicas)
                grad[at, cols] = outer
                if g < EARLY_GROUPS:
                    early[g, 0, 0, at, pl.ds(c, BLOCK)] = outer.astype(jnp.bfloat16)
                square = outer * outer
                for s in range(0, tile, 8):
                    squares += square[s : s + 8]
            return squares

        return lax.fori_loop(0, rows // tile, add, squares)

    def early_first(g, part):
        for dq in range(1, spans(g)[1]):
            copy_early(g, part, 0, dq, 0).start()

    def early_second(g, part, source):
        for dp in range(1, spans(g)[0]):
            copy_early(g, part, dp, 0, source).start()

    momentum_load.wait()
    for g in range(EARLY_GROUPS):
        @pl.loop(0, rows // tile)
        def _(t):
            at = pl.ds(pl.multiple_of(t * tile, tile), tile)
            early[g, 1, 0, at] = momentum_v[at, pl.ds(g * width, width)].astype(jnp.bfloat16)

    ahead = (1,)
    squares = jnp.zeros((8, BLOCK), jnp.float32)
    for g in range(EARLY_GROUPS):
        squares = add_group(g, squares)
        for part in ahead:
            early_first(g, part)
    for g in range(EARLY_GROUPS, groups):
        squares = add_group(g, squares)

    square_mine[...] = squares
    square_near[0] = squares
    for step in range(1, replicas):
        pltpu.make_async_remote_copy(
            src_ref=square_mine, dst_ref=square_near.at[step],
            send_sem=square_sems.at[0], recv_sem=square_sems.at[1],
            device_id={"replica": near(step)}, device_id_type=MESH,
        ).start()
    for g in range(EARLY_GROUPS):
        for part in (1, 0):
            if part not in ahead:
                early_first(g, part)
    for g in range(EARLY_GROUPS):
        for part in (1, 0):
            early_second(g, part, 0)

    arrived(square_near.at[pl.ds(1, replicas - 1)], square_sems.at[1])
    squares = square_near[me]
    for at in range(1, replicas):
        squares += square_near[lax.rem(me + replicas - at, replicas)]
    square_row[...] = squares
    square_far[0] = squares
    for step in range(1, shards_count):
        pltpu.make_async_remote_copy(
            src_ref=square_row, dst_ref=square_far.at[step],
            send_sem=square_sems.at[2], recv_sem=square_sems.at[3],
            device_id={"fsdp": far(step)}, device_id_type=MESH,
        ).start()

    for g in range(EARLY_GROUPS):
        np, nq = spans(g)
        for dq in range(1, nq):
            for part in (1, 0):
                copy_early(g, part, 0, (nq - dq) % nq, 0).wait_recv()
                early_second(g, part, dq)

    def pass_on(g):
        np, nq = spans(g)
        for dq in range(1, nq):
            copy_all(g, 0, (nq - dq) % nq, 0).wait_recv()
            for dp in range(1, np):
                copy_all(g, dp, 0, dq).start()

    arrived(square_far.at[pl.ds(1, shards_count - 1)], square_sems.at[3])
    squares = square_far[row_me]
    for at in range(1, shards_count):
        squares += square_far[lax.rem(row_me + shards_count - at, shards_count)]
    mean_square = jnp.full((1, BLOCK), jnp.sum(squares), jnp.float32) / total
    clip_factor = jnp.minimum(1.0, clip_rms / jnp.sqrt(mean_square + epsilon))

    def moved_and_change(outer, kept):
        step_term = clip_factor * outer
        moved = outer_momentum * kept + step_term
        return moved, step_term + outer_momentum * moved

    def advance(g):
        @pl.loop(0, rows // tile)
        def _(t):
            at = pl.ds(pl.multiple_of(t * tile, tile), tile)
            for c in range(0, width, BLOCK):
                cols = pl.ds(g * width + c, BLOCK)
                moved, change = moved_and_change(grad[at, cols], momentum_v[at, cols])
                new_momentum[at, cols] = moved
                if g >= EARLY_GROUPS:
                    update[g, 0, at, pl.ds(c, BLOCK)] = change.astype(jnp.bfloat16)

    for g in range(EARLY_GROUPS, groups):
        advance(g)
        for dq in range(1, spans(g)[1]):
            copy_all(g, 0, dq, 0).start()
    for g in range(EARLY_GROUPS, groups):
        for dp in range(1, spans(g)[0]):
            copy_all(g, dp, 0, 0).start()

    def finish(g, dp, dq):
        slot = dp * spans(g)[1] + dq
        start = row_start(owner(g, dp, dq))

        @pl.loop(0, rows // tile)
        def _(t):
            at = pl.ds(pl.multiple_of(start + t * tile, tile), tile)
            to = pl.ds(pl.multiple_of(t * tile, tile), tile)
            for c in range(0, width, BLOCK):
                cols = pl.ds(g * width + c, BLOCK)
                from_cols = pl.ds(c, BLOCK)
                if g < EARLY_GROUPS:
                    _, change = moved_and_change(
                        early[g, 0, slot, to, from_cols].astype(jnp.float32),
                        early[g, 1, slot, to, from_cols].astype(jnp.float32),
                    )
                else:
                    change = update[g, slot, to, from_cols].astype(jnp.float32)
                fresh = base_v[at, cols] - outer_rate * change
                new_base[at, cols] = fresh
                blended = blend_share * inner_v[at, cols].astype(jnp.float32) + (
                    1.0 - blend_share
                ) * fresh
                new_inner[0, at, cols] = blended.astype(jnp.bfloat16)

    def finish_last(g, dq):
        np = spans(g)[0]
        for dp in range(1, np):
            if g < EARLY_GROUPS:
                for part in range(2):
                    copy_early(g, part, (np - dp) % np, 0, dq).wait_recv()
            else:
                copy_all(g, (np - dp) % np, 0, dq).wait_recv()
            finish(g, dp, dq)

    for g in range(EARLY_GROUPS):
        advance(g)
        for dq in range(spans(g)[1]):
            finish(g, 0, dq)
    for g in range(EARLY_GROUPS, groups):
        finish(g, 0, 0)
    for g in range(EARLY_GROUPS, groups):
        pass_on(g)
    for g in range(EARLY_GROUPS, groups):
        for dq in range(1, spans(g)[1]):
            finish(g, 0, dq)
    for dq in range(most):
        for g in range(groups):
            if dq < spans(g)[1]:
                finish_last(g, dq)
    others = pl.ds(0, replicas - 1)
    arrived(dec.at[:, others], send_sems.at[0])
    arrived(update.at[pl.ds(0, groups - EARLY_GROUPS), others], send_sems.at[1])
    arrived(early.at[:, :, others], send_sems.at[2])
    arrived(square_near.at[others], square_sems.at[0])
    arrived(square_far.at[pl.ds(0, shards_count - 1)], square_sems.at[2])


def write_out(*refs):
    sems = refs[-1]
    parts = len(refs) // 2
    copies = [
        pltpu.make_async_copy(refs[i], refs[parts + i], sems.at[i]) for i in range(parts)
    ]
    for copy in copies:
        copy.start()
    for copy in copies:
        copy.wait()


def shards(base_weights, inner_weights, momentum):
    replicas = lax.axis_size("replica")
    shards_count = lax.axis_size("fsdp")
    local_rows, columns = base_weights.shape
    rows = local_rows // replicas
    groups = 2 * HALF_GROUPS
    width = columns // groups
    total = float(local_rows * shards_count * columns)
    dims = (replicas, shards_count, rows, columns, groups, total)
    most = max(grid_sides(replicas))
    dma = pltpu.SemaphoreType.DMA
    blocks = (groups, replicas, rows, width)
    outside = pl.BlockSpec(memory_space=pltpu.HBM)
    vmem = pl.BlockSpec(memory_space=pltpu.VMEM)
    in_hbm = functools.partial(pltpu.with_memory_space_constraint, memory_space=pltpu.HBM)
    in_vmem = functools.partial(pltpu.with_memory_space_constraint, memory_space=pltpu.VMEM)
    held = pl.pallas_call(
        functools.partial(kernel, dims),
        out_shape=(
            pltpu.VMEM(base_weights.shape, jnp.float32),
            pltpu.VMEM(momentum.shape, jnp.float32),
            pltpu.VMEM(inner_weights.shape, jnp.bfloat16),
        ),
        in_specs=[outside] * 3,
        out_specs=(vmem, vmem, vmem),
        scratch_shapes=[
            pltpu.VMEM((local_rows, columns), jnp.float32),
            pltpu.VMEM((local_rows, columns), jnp.bfloat16),
            pltpu.VMEM((rows, columns), jnp.float32),
            pltpu.VMEM(blocks, jnp.bfloat16),
            pltpu.VMEM(blocks, jnp.bfloat16),
            pltpu.VMEM((groups, most, rows, width), jnp.bfloat16),
            pltpu.VMEM((rows, columns), jnp.float32),
            pltpu.VMEM(blocks, jnp.bfloat16),
            pltpu.VMEM((EARLY_GROUPS, 2, replicas, rows, width), jnp.bfloat16),
            pltpu.VMEM((8, BLOCK), jnp.float32),
            pltpu.VMEM((replicas, 8, BLOCK), jnp.float32),
            pltpu.VMEM((8, BLOCK), jnp.float32),
            pltpu.VMEM((shards_count, 8, BLOCK), jnp.float32),
            dma((replicas + 1, 2)),
            dma((3,)),
            dma((groups, replicas - 1)),
            dma((EARLY_GROUPS, 2, replicas - 1)),
            dma((4,)),
            pltpu.SemaphoreType.REGULAR((1,)),
        ],
        compiler_params=pltpu.CompilerParams(collective_id=0, has_side_effects=True, vmem_limit_bytes=36 * 2**20),
    )(in_hbm(base_weights), in_hbm(inner_weights), in_hbm(momentum))
    return pl.pallas_call(
        write_out,
        out_shape=tuple(jax.ShapeDtypeStruct(part.shape, part.dtype) for part in held),
        in_specs=[vmem] * len(held),
        out_specs=tuple(outside for part in held),
        scratch_shapes=[dma((len(held),))],
        compiler_params=pltpu.CompilerParams(vmem_limit_bytes=2**20),
    )(*[in_vmem(part) for part in held])


def solution(mesh):
    placed = (P("fsdp", None), P("replica", "fsdp", None), P(("fsdp", "replica"), None))
    return jax.shard_map(
        shards,
        mesh=mesh,
        in_specs=placed,
        out_specs=(P("fsdp", None), P(("fsdp", "replica"), None), P("replica", "fsdp", None)),
        check_vma=False,
    )
```

```python
import functools

import jax
import jax.numpy as jnp
from jax import lax
from jax.experimental import pallas as pl
from jax.experimental.pallas import tpu as pltpu
from jax.sharding import PartitionSpec as P

BLOCK = 128
HALF_GROUPS = 4
EARLY_GROUPS = 2
ENCODE_ROWS = 256
PLAIN_ROWS = 128

code_limit = 448.0
outer_rate = 0.7
outer_momentum = 0.9
blend_share = 0.5
clip_rms = 0.02
epsilon = 1e-06

MESH = pl.DeviceIdType.MESH


def decoded_deltas(deltas):
    peaks = jnp.max(jnp.abs(deltas), axis=1, keepdims=True) + epsilon
    rough = peaks * (1.0 / code_limit)
    wide = rough * (2.0**23 + 1.0)
    power = wide - (wide - rough)
    scales = jnp.where(power * code_limit < peaks, power + power, power)
    nudged = deltas * (1.0 + 2.0**-23)
    wide_deltas = nudged * (2.0**20 + 1.0)
    four_bits = wide_deltas - (wide_deltas - nudged)
    shift = scales * (1.5 * 2.0**14)
    fixed_step = (nudged + shift) - shift
    return jnp.where(jnp.abs(deltas) < scales * 2.0**-6, fixed_step, four_bits)


def arrived(blocks, sem):
    pltpu.make_async_copy(blocks, blocks, sem).wait()


def grid_sides(replicas):
    side = 1 << (replicas.bit_length() // 2)
    while replicas % side:
        side -= 1
    return side, replicas // side


def rounds(count):
    return max(count - 2, 0).bit_length()


def kernel(
    dims,
    base_hbm, inner_hbm, momentum_hbm,
    new_base, new_momentum, new_inner,
    base_v, inner_v, momentum_v, dec, first, second, grad, update, early,
    square_mine, square_all,
    load_sems, send_sems, recv_sems, early_sems, square_sems, entry_sems,
):
    replicas, shards_count, rows, columns, groups, total = dims
    width = columns // groups
    span_x, span_y = grid_sides(replicas)
    tile = min(PLAIN_ROWS, rows)
    encode_tile = min(ENCODE_ROWS, rows)
    me = lax.axis_index("replica")
    row_me = lax.axis_index("fsdp")
    me_x, me_y = lax.rem(me, span_x), me // span_x

    def spans(g):
        return (span_x, span_y) if g % 2 == 0 else (span_y, span_x)

    def owner(g, dp, dq):
        dx, dy = (dp, dq) if g % 2 == 0 else (dq, dp)
        return lax.rem(me_y + dy, span_y) * span_x + lax.rem(me_x + dx, span_x)

    def near(step):
        return lax.rem(me + step, replicas)

    def far(step):
        return lax.rem(row_me + step, shards_count)

    def row_start(index):
        return pl.multiple_of(index * rows, rows)

    def greet(sem, step):
        @pl.when(row_me >= step)
        def _():
            pl.semaphore_signal(sem, inc=1, device_id={"fsdp": row_me - step}, device_id_type=MESH)

        @pl.when(row_me + step < shards_count)
        def _():
            pl.semaphore_signal(sem, inc=1, device_id={"fsdp": row_me + step}, device_id_type=MESH)

    def greeters(step):
        below = jnp.where(row_me >= step, 1, 0)
        return below + jnp.where(row_me + step < shards_count, 1, 0)

    barrier = pltpu.get_barrier_semaphore()
    for step in range(1, replicas):
        pl.semaphore_signal(barrier, inc=1, device_id={"replica": near(step)}, device_id_type=MESH)
    greet(barrier, 1)

    load_order = [(dx, dy) for dy in reversed(range(span_y)) for dx in reversed(range(span_x))]
    loads = []
    for at, (dx, dy) in enumerate(load_order):
        here = pl.ds(row_start(owner(0, dx, dy)), rows)
        pair = (
            pltpu.make_async_copy(base_hbm.at[here], base_v.at[here], load_sems.at[at, 0]),
            pltpu.make_async_copy(inner_hbm.at[0, here], inner_v.at[here], load_sems.at[at, 1]),
        )
        for copy in pair:
            copy.start()
        loads.append(pair)
    momentum_load = pltpu.make_async_copy(momentum_hbm, momentum_v, load_sems.at[replicas, 0])
    momentum_load.start()

    def encode(g, dp, dq):
        slot = dp * spans(g)[1] + dq
        start = row_start(owner(g, dp, dq))

        @pl.loop(0, rows // encode_tile)
        def _(t):
            at = pl.ds(pl.multiple_of(start + t * encode_tile, encode_tile), encode_tile)
            to = pl.ds(pl.multiple_of(t * encode_tile, encode_tile), encode_tile)
            for c in range(0, width, BLOCK):
                cols = pl.ds(g * width + c, BLOCK)
                deltas = base_v[at, cols] - inner_v[at, cols].astype(jnp.float32)
                dec[g, slot, to, pl.ds(c, BLOCK)] = decoded_deltas(deltas).astype(jnp.bfloat16)

    def copy_one(g, dp, dq):
        slot = dp * spans(g)[1] + dq
        return pltpu.make_async_remote_copy(
            src_ref=dec.at[g, slot], dst_ref=first.at[g, slot],
            send_sem=send_sems.at[0], recv_sem=recv_sems.at[g, slot - 1],
            device_id={"replica": owner(g, dp, 0)}, device_id_type=MESH,
        )

    def copy_two(g, dq):
        return pltpu.make_async_remote_copy(
            src_ref=dec.at[g, dq], dst_ref=second.at[g, dq],
            send_sem=send_sems.at[0], recv_sem=recv_sems.at[g, dq - 1],
            device_id={"replica": owner(g, 0, dq)}, device_id_type=MESH,
        )

    def arrival(g, dp, dq, source):
        np, nq = spans(g)
        return ((np - dp) % np) * nq + (source if dp else (nq - dq) % nq)

    def copy_all(g, dp, dq, source):
        slot = arrival(g, dp, dq, source)
        return pltpu.make_async_remote_copy(
            src_ref=update.at[g, source if dp else 0], dst_ref=update.at[g, slot],
            send_sem=send_sems.at[1], recv_sem=recv_sems.at[g, slot - 1],
            device_id={"replica": owner(g, dp, dq)}, device_id_type=MESH,
        )

    def copy_early(g, part, dp, dq, source):
        slot = arrival(g, dp, dq, source)
        return pltpu.make_async_remote_copy(
            src_ref=early.at[g, part, source if dp else 0], dst_ref=early.at[g, part, slot],
            send_sem=send_sems.at[2], recv_sem=early_sems.at[g, part, slot - 1],
            device_id={"replica": owner(g, dp, dq)}, device_id_type=MESH,
        )

    waited = set()

    def await_load(g, dp, dq):
        key = (dp, dq) if g % 2 == 0 else (dq, dp)
        if key not in waited:
            waited.add(key)
            for copy in loads[load_order.index(key)]:
                copy.wait()

    greeted = False
    most = max(span_x, span_y)
    for dq in reversed(range(most)):
        for dp in reversed(range(1, most)):
            for g in range(groups):
                np, nq = spans(g)
                if dp < np and dq < nq:
                    await_load(g, dp, dq)
                    encode(g, dp, dq)
                    if not greeted:
                        pl.semaphore_wait(barrier, replicas - 1 + greeters(1))
                        greeted = True
                    copy_one(g, dp, dq).start()
    for at in range(rounds(shards_count)):
        greet(entry_sems.at[at], 1 << at)
        pl.semaphore_wait(entry_sems.at[at], greeters(1 << at))
    for step in range(1, replicas):
        pl.semaphore_signal(entry_sems.at[rounds(shards_count)], inc=1, device_id={"replica": near(step)}, device_id_type=MESH)
    for dq in reversed(range(most)):
        for g in range(groups):
            if dq < spans(g)[1]:
                await_load(g, 0, dq)
                encode(g, 0, dq)

    for dq in reversed(range(most)):
        for g in range(groups):
            np, nq = spans(g)
            if dq >= nq:
                continue
            for dp in range(1, np):
                copy_one(g, dp, dq).wait_recv()

            @pl.loop(0, rows // tile)
            def _(t):
                at = pl.ds(pl.multiple_of(t * tile, tile), tile)
                summed = dec[g, dq, at].astype(jnp.float32)
                for dp in range(1, np):
                    summed += first[g, dp * nq + dq, at].astype(jnp.float32)
                if dq:
                    dec[g, dq, at] = summed.astype(jnp.bfloat16)
                else:
                    grad[at, pl.ds(g * width, width)] = summed

            if dq:
                copy_two(g, dq).start()

    def add_group(g, squares):
        nq = spans(g)[1]
        for dq in range(1, nq):
            copy_two(g, dq).wait_recv()

        def add(t, squares):
            at = pl.ds(pl.multiple_of(t * tile, tile), tile)
            for c in range(0, width, BLOCK):
                cols = pl.ds(g * width + c, BLOCK)
                summed = grad[at, cols]
                for dq in range(1, nq):
                    summed += second[g, dq, at, pl.ds(c, BLOCK)].astype(jnp.float32)
                outer = summed * (1.0 / replicas)
                grad[at, cols] = outer
                if g < EARLY_GROUPS:
                    early[g, 0, 0, at, pl.ds(c, BLOCK)] = outer.astype(jnp.bfloat16)
                square = outer * outer
                for s in range(0, tile, 8):
                    squares += square[s : s + 8]
            return squares

        return lax.fori_loop(0, rows // tile, add, squares)

    def early_first(g, part):
        for dq in range(1, spans(g)[1]):
            copy_early(g, part, 0, dq, 0).start()

    def early_second(g, part, source):
        for dp in range(1, spans(g)[0]):
            copy_early(g, part, dp, 0, source).start()

    momentum_load.wait()
    for g in range(EARLY_GROUPS):
        @pl.loop(0, rows // tile)
        def _(t):
            at = pl.ds(pl.multiple_of(t * tile, tile), tile)
            early[g, 1, 0, at] = momentum_v[at, pl.ds(g * width, width)].astype(jnp.bfloat16)

    ahead = (1, 0)
    squares = jnp.zeros((8, BLOCK), jnp.float32)
    for g in range(EARLY_GROUPS):
        squares = add_group(g, squares)
        for part in ahead:
            early_first(g, part)
    for g in range(EARLY_GROUPS, groups):
        squares = add_group(g, squares)

    spot = row_me * replicas + me
    square_row = jnp.sum(squares, axis=0, keepdims=True)
    square_mine[...] = square_row
    square_all[spot] = square_row
    pl.semaphore_wait(entry_sems.at[rounds(shards_count)], replicas - 1)
    def send_square(step, hop):
        pltpu.make_async_remote_copy(
            src_ref=square_mine, dst_ref=square_all.at[spot],
            send_sem=square_sems.at[0], recv_sem=square_sems.at[1],
            device_id={"replica": near(step), "fsdp": far(hop)}, device_id_type=MESH,
        ).start()

    for step in reversed(range(replicas)):
        @pl.loop(0 if step else 1, shards_count)
        def _(hop):
            send_square(step, hop)

    for g in range(EARLY_GROUPS):
        for part in (1, 0):
            if part not in ahead:
                early_first(g, part)
    for g in range(EARLY_GROUPS):
        for part in (1, 0):
            early_second(g, part, 0)

    for g in range(EARLY_GROUPS):
        np, nq = spans(g)
        for dq in range(1, nq):
            for part in (1, 0):
                copy_early(g, part, 0, (nq - dq) % nq, 0).wait_recv()
                early_second(g, part, dq)

    def pass_on(g):
        np, nq = spans(g)
        for dq in range(1, nq):
            copy_all(g, 0, (nq - dq) % nq, 0).wait_recv()
            for dp in range(1, np):
                copy_all(g, dp, 0, dq).start()

    everyone = pl.ds(0, shards_count * replicas - 1)
    arrived(square_all.at[everyone], square_sems.at[1])
    squares = jnp.sum(square_all[...], axis=0)
    mean_square = jnp.full((1, BLOCK), jnp.sum(squares), jnp.float32) / total
    clip_factor = jnp.minimum(1.0, clip_rms / jnp.sqrt(mean_square + epsilon))

    def moved_and_change(outer, kept):
        step_term = clip_factor * outer
        moved = outer_momentum * kept + step_term
        return moved, step_term + outer_momentum * moved

    def advance(g):
        @pl.loop(0, rows // tile)
        def _(t):
            at = pl.ds(pl.multiple_of(t * tile, tile), tile)
            for c in range(0, width, BLOCK):
                cols = pl.ds(g * width + c, BLOCK)
                moved, change = moved_and_change(grad[at, cols], momentum_v[at, cols])
                new_momentum[at, cols] = moved
                if g >= EARLY_GROUPS:
                    update[g, 0, at, pl.ds(c, BLOCK)] = change.astype(jnp.bfloat16)

    for g in range(EARLY_GROUPS, groups):
        advance(g)
        for dq in range(1, spans(g)[1]):
            copy_all(g, 0, dq, 0).start()
    for g in range(EARLY_GROUPS, groups):
        for dp in range(1, spans(g)[0]):
            copy_all(g, dp, 0, 0).start()

    def finish(g, dp, dq):
        slot = dp * spans(g)[1] + dq
        start = row_start(owner(g, dp, dq))

        @pl.loop(0, rows // tile)
        def _(t):
            at = pl.ds(pl.multiple_of(start + t * tile, tile), tile)
            to = pl.ds(pl.multiple_of(t * tile, tile), tile)
            for c in range(0, width, BLOCK):
                cols = pl.ds(g * width + c, BLOCK)
                from_cols = pl.ds(c, BLOCK)
                if g < EARLY_GROUPS:
                    _, change = moved_and_change(
                        early[g, 0, slot, to, from_cols].astype(jnp.float32),
                        early[g, 1, slot, to, from_cols].astype(jnp.float32),
                    )
                else:
                    change = update[g, slot, to, from_cols].astype(jnp.float32)
                fresh = base_v[at, cols] - outer_rate * change
                new_base[at, cols] = fresh
                blended = blend_share * inner_v[at, cols].astype(jnp.float32) + (
                    1.0 - blend_share
                ) * fresh
                new_inner[0, at, cols] = blended.astype(jnp.bfloat16)

    def finish_last(g, dq):
        np = spans(g)[0]
        for dp in range(1, np):
            if g < EARLY_GROUPS:
                for part in range(2):
                    copy_early(g, part, (np - dp) % np, 0, dq).wait_recv()
            else:
                copy_all(g, (np - dp) % np, 0, dq).wait_recv()
            finish(g, dp, dq)

    for g in range(EARLY_GROUPS):
        advance(g)
        for dq in range(spans(g)[1]):
            finish(g, 0, dq)
    for g in range(EARLY_GROUPS, groups):
        finish(g, 0, 0)
    for g in range(EARLY_GROUPS, groups):
        pass_on(g)
    for g in range(EARLY_GROUPS, groups):
        for dq in range(1, spans(g)[1]):
            finish(g, 0, dq)
    for dq in range(most):
        for g in range(groups):
            if dq < spans(g)[1]:
                finish_last(g, dq)
    others = pl.ds(0, replicas - 1)
    arrived(dec.at[:, others], send_sems.at[0])
    arrived(update.at[pl.ds(0, groups - EARLY_GROUPS), others], send_sems.at[1])
    arrived(early.at[:, :, others], send_sems.at[2])
    arrived(square_all.at[everyone], square_sems.at[0])


def write_out(*refs):
    sems = refs[-1]
    parts = len(refs) // 2
    copies = [
        pltpu.make_async_copy(refs[i], refs[parts + i], sems.at[i]) for i in range(parts)
    ]
    for copy in copies:
        copy.start()
    for copy in copies:
        copy.wait()


def shards(base_weights, inner_weights, momentum):
    replicas = lax.axis_size("replica")
    shards_count = lax.axis_size("fsdp")
    local_rows, columns = base_weights.shape
    rows = local_rows // replicas
    groups = 2 * HALF_GROUPS
    width = columns // groups
    total = float(local_rows * shards_count * columns)
    dims = (replicas, shards_count, rows, columns, groups, total)
    most = max(grid_sides(replicas))
    dma = pltpu.SemaphoreType.DMA
    blocks = (groups, replicas, rows, width)
    outside = pl.BlockSpec(memory_space=pltpu.HBM)
    vmem = pl.BlockSpec(memory_space=pltpu.VMEM)
    in_hbm = functools.partial(pltpu.with_memory_space_constraint, memory_space=pltpu.HBM)
    in_vmem = functools.partial(pltpu.with_memory_space_constraint, memory_space=pltpu.VMEM)
    held = pl.pallas_call(
        functools.partial(kernel, dims),
        out_shape=(
            pltpu.VMEM(base_weights.shape, jnp.float32),
            pltpu.VMEM(momentum.shape, jnp.float32),
            pltpu.VMEM(inner_weights.shape, jnp.bfloat16),
        ),
        in_specs=[outside] * 3,
        out_specs=(vmem, vmem, vmem),
        scratch_shapes=[
            pltpu.VMEM((local_rows, columns), jnp.float32),
            pltpu.VMEM((local_rows, columns), jnp.bfloat16),
            pltpu.VMEM((rows, columns), jnp.float32),
            pltpu.VMEM(blocks, jnp.bfloat16),
            pltpu.VMEM(blocks, jnp.bfloat16),
            pltpu.VMEM((groups, most, rows, width), jnp.bfloat16),
            pltpu.VMEM((rows, columns), jnp.float32),
            pltpu.VMEM(blocks, jnp.bfloat16),
            pltpu.VMEM((EARLY_GROUPS, 2, replicas, rows, width), jnp.bfloat16),
            pltpu.VMEM((1, BLOCK), jnp.float32),
            pltpu.VMEM((shards_count * replicas, 1, BLOCK), jnp.float32),
            dma((replicas + 1, 2)),
            dma((3,)),
            dma((groups, replicas - 1)),
            dma((EARLY_GROUPS, 2, replicas - 1)),
            dma((2,)),
            pltpu.SemaphoreType.REGULAR((rounds(shards_count) + 1,)),
        ],
        compiler_params=pltpu.CompilerParams(collective_id=0, has_side_effects=True, vmem_limit_bytes=36 * 2**20),
    )(in_hbm(base_weights), in_hbm(inner_weights), in_hbm(momentum))
    return pl.pallas_call(
        write_out,
        out_shape=tuple(jax.ShapeDtypeStruct(part.shape, part.dtype) for part in held),
        in_specs=[vmem] * len(held),
        out_specs=tuple(outside for part in held),
        scratch_shapes=[dma((len(held),))],
        compiler_params=pltpu.CompilerParams(vmem_limit_bytes=2**20),
    )(*[in_vmem(part) for part in held])


def solution(mesh):
    placed = (P("fsdp", None), P("replica", "fsdp", None), P(("fsdp", "replica"), None))
    return jax.shard_map(
        shards,
        mesh=mesh,
        in_specs=placed,
        out_specs=(P("fsdp", None), P(("fsdp", "replica"), None), P("replica", "fsdp", None)),
        check_vma=False,
    )
```

```python
import functools

import jax
import jax.numpy as jnp
from jax import lax
from jax.experimental import pallas as pl
from jax.experimental.pallas import tpu as pltpu
from jax.sharding import PartitionSpec as P

BLOCK = 128
HALF_GROUPS = 4
EARLY_GROUPS = 2
ENCODE_ROWS = 256
FIRST_GROUPS = 2
PLAIN_ROWS = 128

code_limit = 448.0
outer_rate = 0.7
outer_momentum = 0.9
blend_share = 0.5
clip_rms = 0.02
epsilon = 1e-06

MESH = pl.DeviceIdType.MESH


def decoded_deltas(deltas):
    peaks = jnp.max(jnp.abs(deltas), axis=1, keepdims=True) + epsilon
    rough = peaks * (1.0 / code_limit)
    wide = rough * (2.0**23 + 1.0)
    power = wide - (wide - rough)
    scales = jnp.where(power * code_limit < peaks, power + power, power)
    nudged = deltas * (1.0 + 2.0**-23)
    wide_deltas = nudged * (2.0**20 + 1.0)
    four_bits = wide_deltas - (wide_deltas - nudged)
    shift = scales * (1.5 * 2.0**14)
    fixed_step = (nudged + shift) - shift
    return jnp.where(jnp.abs(deltas) < scales * 2.0**-6, fixed_step, four_bits)


def arrived(blocks, sem):
    pltpu.make_async_copy(blocks, blocks, sem).wait()


def grid_sides(replicas):
    side = 1 << (replicas.bit_length() // 2)
    while replicas % side:
        side -= 1
    return side, replicas // side


def rounds(count):
    return max(count - 2, 0).bit_length()


def kernel(
    dims,
    base_hbm, inner_hbm, momentum_hbm,
    new_base, new_momentum, new_inner,
    base_v, inner_v, momentum_v, dec, first, second, grad, update, early,
    square_mine, square_all,
    load_sems, send_sems, recv_sems, early_sems, square_sems, entry_sems,
):
    replicas, shards_count, rows, columns, groups, total = dims
    width = columns // groups
    span_x, span_y = grid_sides(replicas)
    tile = min(PLAIN_ROWS, rows)
    encode_tile = min(ENCODE_ROWS, rows)
    me = lax.axis_index("replica")
    row_me = lax.axis_index("fsdp")
    me_x, me_y = lax.rem(me, span_x), me // span_x

    def spans(g):
        return (span_x, span_y) if g % 2 == 0 else (span_y, span_x)

    def owner(g, dp, dq):
        dx, dy = (dp, dq) if g % 2 == 0 else (dq, dp)
        return lax.rem(me_y + dy, span_y) * span_x + lax.rem(me_x + dx, span_x)

    def near(step):
        return lax.rem(me + step, replicas)

    def far(step):
        return lax.rem(row_me + step, shards_count)

    def row_start(index):
        return pl.multiple_of(index * rows, rows)

    def greet(sem, step):
        @pl.when(row_me >= step)
        def _():
            pl.semaphore_signal(sem, inc=1, device_id={"fsdp": row_me - step}, device_id_type=MESH)

        @pl.when(row_me + step < shards_count)
        def _():
            pl.semaphore_signal(sem, inc=1, device_id={"fsdp": row_me + step}, device_id_type=MESH)

    def greeters(step):
        below = jnp.where(row_me >= step, 1, 0)
        return below + jnp.where(row_me + step < shards_count, 1, 0)

    barrier = pltpu.get_barrier_semaphore()
    beside = [owner(0, dx, 0) for dx in range(1, span_x)]
    above = [owner(0, 0, dy) for dy in range(1, span_y)]
    load_order = [(dx, dy) for dy in reversed(range(span_y)) for dx in reversed(range(span_x))]
    pieces = []
    for dx, dy in load_order:
        cuts = [0, columns] if pieces else [0, FIRST_GROUPS * width, columns]
        pieces += [((dx, dy), low, high) for low, high in zip(cuts, cuts[1:])]

    def load(at):
        (dx, dy), low, high = pieces[at]
        here = pl.ds(row_start(owner(0, dx, dy)), rows)
        cols = pl.ds(low, high - low)
        pltpu.make_async_copy(base_hbm.at[here, cols], base_v.at[here, cols], load_sems.at[at]).start()
        pltpu.make_async_copy(inner_hbm.at[0, here, cols], inner_v.at[here, cols], load_sems.at[at]).start()

    load(0)
    for peer in beside + above:
        pl.semaphore_signal(barrier, inc=1, device_id={"replica": peer}, device_id_type=MESH)
    greet(barrier, 1)
    for at in range(1, len(pieces)):
        load(at)
    momentum_load = pltpu.make_async_copy(momentum_hbm, momentum_v, load_sems.at[replicas + 1])
    momentum_load.start()

    def encode(g, dp, dq):
        slot = dp * spans(g)[1] + dq
        start = row_start(owner(g, dp, dq))

        @pl.loop(0, rows // encode_tile)
        def _(t):
            at = pl.ds(pl.multiple_of(start + t * encode_tile, encode_tile), encode_tile)
            to = pl.ds(pl.multiple_of(t * encode_tile, encode_tile), encode_tile)
            for c in range(0, width, BLOCK):
                cols = pl.ds(g * width + c, BLOCK)
                deltas = base_v[at, cols] - inner_v[at, cols].astype(jnp.float32)
                dec[g, slot, to, pl.ds(c, BLOCK)] = decoded_deltas(deltas).astype(jnp.bfloat16)

    def copy_one(g, dp, dq):
        slot = dp * spans(g)[1] + dq
        return pltpu.make_async_remote_copy(
            src_ref=dec.at[g, slot], dst_ref=first.at[g, slot],
            send_sem=send_sems.at[0], recv_sem=recv_sems.at[g, slot - 1],
            device_id={"replica": owner(g, dp, 0)}, device_id_type=MESH,
        )

    def copy_two(g, dq):
        return pltpu.make_async_remote_copy(
            src_ref=dec.at[g, dq], dst_ref=second.at[g, dq],
            send_sem=send_sems.at[0], recv_sem=recv_sems.at[g, dq - 1],
            device_id={"replica": owner(g, 0, dq)}, device_id_type=MESH,
        )

    def arrival(g, dp, dq, source):
        np, nq = spans(g)
        return ((np - dp) % np) * nq + (source if dp else (nq - dq) % nq)

    def copy_all(g, dp, dq, source):
        slot = arrival(g, dp, dq, source)
        return pltpu.make_async_remote_copy(
            src_ref=update.at[g, source if dp else 0], dst_ref=update.at[g, slot],
            send_sem=send_sems.at[1], recv_sem=recv_sems.at[g, slot - 1],
            device_id={"replica": owner(g, dp, dq)}, device_id_type=MESH,
        )

    def copy_early(g, dp, dq, source):
        slot = arrival(g, dp, dq, source)
        return pltpu.make_async_remote_copy(
            src_ref=early.at[g, source if dp else 0], dst_ref=early.at[g, slot],
            send_sem=send_sems.at[2], recv_sem=early_sems.at[g, slot - 1],
            device_id={"replica": owner(g, dp, dq)}, device_id_type=MESH,
        )

    waited = set()

    def await_load(g, dp, dq):
        key = (dp, dq) if g % 2 == 0 else (dq, dp)
        for at, (where, low, high) in enumerate(pieces):
            if where == key and low <= g * width < high and at not in waited:
                waited.add(at)
                arrived(base_v.at[pl.ds(0, rows + rows // 2), pl.ds(0, high - low)], load_sems.at[at])

    greeted = False
    most = max(span_x, span_y)
    for dq in reversed(range(most)):
        for dp in reversed(range(1, most)):
            for g in range(groups):
                np, nq = spans(g)
                if dp < np and dq < nq:
                    await_load(g, dp, dq)
                    encode(g, dp, dq)
                    if not greeted:
                        pl.semaphore_wait(barrier, len(beside) + len(above) + greeters(1))
                        greeted = True
                    copy_one(g, dp, dq).start()
    def sum_one(g, dq):
        np, nq = spans(g)
        for dp in range(1, np):
            copy_one(g, dp, dq).wait_recv()

        @pl.loop(0, rows // tile)
        def _(t):
            at = pl.ds(pl.multiple_of(t * tile, tile), tile)
            summed = dec[g, dq, at].astype(jnp.float32)
            for dp in range(1, np):
                summed += first[g, dp * nq + dq, at].astype(jnp.float32)
            if dq:
                dec[g, dq, at] = summed.astype(jnp.bfloat16)
            else:
                grad[at, pl.ds(g * width, width)] = summed

        if dq:
            copy_two(g, dq).start()

    line_rounds = rounds(shards_count)

    def call(at):
        if at < line_rounds:
            greet(entry_sems.at[at], 1 << at)
        else:
            for peer in (beside, above)[at - line_rounds]:
                pl.semaphore_signal(entry_sems.at[at], inc=1, device_id={"replica": peer}, device_id_type=MESH)

    def hear(at):
        count = greeters(1 << at) if at < line_rounds else len((beside, above)[at - line_rounds])
        pl.semaphore_wait(entry_sems.at[at], count)

    call(0)
    called = 1
    done = 0
    for dq in reversed(range(most)):
        mine = [g for g in range(groups) if dq < spans(g)[1]]
        for g in mine:
            await_load(g, 0, dq)
            encode(g, 0, dq)
            done += 1
            if done % 4 == 0 and called < line_rounds + 2:
                hear(called - 1)
                call(called)
                called += 1
        for g in mine:
            sum_one(g, dq)
    for at in range(called, line_rounds + 2):
        hear(at - 1)
        call(at)
    hear(line_rounds + 1)

    def add_group(g, squares):
        nq = spans(g)[1]
        for dq in range(1, nq):
            copy_two(g, dq).wait_recv()

        def add(t, squares):
            at = pl.ds(pl.multiple_of(t * tile, tile), tile)
            for c in range(0, width, BLOCK):
                cols = pl.ds(g * width + c, BLOCK)
                summed = grad[at, cols]
                for dq in range(1, nq):
                    summed += second[g, dq, at, pl.ds(c, BLOCK)].astype(jnp.float32)
                outer = summed * (1.0 / replicas)
                grad[at, cols] = outer
                if g < EARLY_GROUPS:
                    early[g, 0, 0, at, pl.ds(c, BLOCK)] = outer.astype(jnp.bfloat16)
                square = outer * outer
                for s in range(0, tile, 8):
                    squares += square[s : s + 8]
            return squares

        return lax.fori_loop(0, rows // tile, add, squares)

    def early_first(g):
        for dq in range(1, spans(g)[1]):
            copy_early(g, 0, dq, 0).start()

    def early_second(g, source):
        for dp in range(1, spans(g)[0]):
            copy_early(g, dp, 0, source).start()

    momentum_load.wait()
    for g in range(EARLY_GROUPS):
        @pl.loop(0, rows // tile)
        def _(t):
            at = pl.ds(pl.multiple_of(t * tile, tile), tile)
            early[g, 0, 1, at] = momentum_v[at, pl.ds(g * width, width)].astype(jnp.bfloat16)

    squares = jnp.zeros((8, BLOCK), jnp.float32)
    for g in range(EARLY_GROUPS):
        squares = add_group(g, squares)
        early_first(g)
    for g in range(EARLY_GROUPS, groups):
        squares = add_group(g, squares)

    spot = row_me * replicas + me
    square_row = jnp.sum(squares, axis=0, keepdims=True)
    square_mine[...] = square_row
    square_all[spot] = square_row
    def send_square(step, row):
        pltpu.make_async_remote_copy(
            src_ref=square_mine, dst_ref=square_all.at[spot],
            send_sem=square_sems.at[0], recv_sem=square_sems.at[1],
            device_id={"replica": near(step), "fsdp": row}, device_id_type=MESH,
        ).start()

    @pl.loop(0, shards_count - 1)
    def _(t):
        at = jnp.where(2 * row_me < shards_count, shards_count - 2 - t, t)
        row = at + jnp.where(at >= row_me, 1, 0)
        for step in reversed(range(replicas)):
            send_square(step, row)

    for step in reversed(range(1, replicas)):
        send_square(step, row_me)

    for g in range(EARLY_GROUPS):
        early_second(g, 0)
    for g in range(EARLY_GROUPS):
        nq = spans(g)[1]
        for dq in range(1, nq):
            copy_early(g, 0, (nq - dq) % nq, 0).wait_recv()
            early_second(g, dq)

    def pass_on(g):
        np, nq = spans(g)
        for dq in range(1, nq):
            copy_all(g, 0, (nq - dq) % nq, 0).wait_recv()
            for dp in range(1, np):
                copy_all(g, dp, 0, dq).start()

    everyone = pl.ds(0, shards_count * replicas - 1)
    arrived(square_all.at[everyone], square_sems.at[1])
    squares = jnp.sum(square_all[...], axis=0)
    mean_square = jnp.full((1, BLOCK), jnp.sum(squares), jnp.float32) / total
    clip_factor = jnp.minimum(1.0, clip_rms / jnp.sqrt(mean_square + epsilon))

    def moved_and_change(outer, kept):
        step_term = clip_factor * outer
        moved = outer_momentum * kept + step_term
        return moved, step_term + outer_momentum * moved

    def advance(g):
        @pl.loop(0, rows // tile)
        def _(t):
            at = pl.ds(pl.multiple_of(t * tile, tile), tile)
            for c in range(0, width, BLOCK):
                cols = pl.ds(g * width + c, BLOCK)
                moved, change = moved_and_change(grad[at, cols], momentum_v[at, cols])
                new_momentum[at, cols] = moved
                if g >= EARLY_GROUPS:
                    update[g, 0, at, pl.ds(c, BLOCK)] = change.astype(jnp.bfloat16)

    for g in range(EARLY_GROUPS, groups):
        advance(g)
        for dq in range(1, spans(g)[1]):
            copy_all(g, 0, dq, 0).start()
    for g in range(EARLY_GROUPS, groups):
        for dp in range(1, spans(g)[0]):
            copy_all(g, dp, 0, 0).start()

    def finish(g, dp, dq):
        slot = dp * spans(g)[1] + dq
        start = row_start(owner(g, dp, dq))

        @pl.loop(0, rows // tile)
        def _(t):
            at = pl.ds(pl.multiple_of(start + t * tile, tile), tile)
            to = pl.ds(pl.multiple_of(t * tile, tile), tile)
            for c in range(0, width, BLOCK):
                cols = pl.ds(g * width + c, BLOCK)
                from_cols = pl.ds(c, BLOCK)
                if g < EARLY_GROUPS:
                    _, change = moved_and_change(
                        early[g, slot, 0, to, from_cols].astype(jnp.float32),
                        early[g, slot, 1, to, from_cols].astype(jnp.float32),
                    )
                else:
                    change = update[g, slot, to, from_cols].astype(jnp.float32)
                fresh = base_v[at, cols] - outer_rate * change
                new_base[at, cols] = fresh
                blended = blend_share * inner_v[at, cols].astype(jnp.float32) + (
                    1.0 - blend_share
                ) * fresh
                new_inner[0, at, cols] = blended.astype(jnp.bfloat16)

    def finish_last(g, dq):
        np = spans(g)[0]
        for dp in range(1, np):
            if g < EARLY_GROUPS:
                copy_early(g, (np - dp) % np, 0, dq).wait_recv()
            else:
                copy_all(g, (np - dp) % np, 0, dq).wait_recv()
            finish(g, dp, dq)

    for g in range(EARLY_GROUPS):
        advance(g)
        for dq in range(spans(g)[1]):
            finish(g, 0, dq)
    for g in range(EARLY_GROUPS, groups):
        finish(g, 0, 0)
    for g in range(EARLY_GROUPS, groups):
        pass_on(g)
    for g in range(EARLY_GROUPS, groups):
        for dq in range(1, spans(g)[1]):
            finish(g, 0, dq)
    for dq in range(most):
        for g in range(groups):
            if dq < spans(g)[1]:
                finish_last(g, dq)
    others = pl.ds(0, replicas - 1)
    arrived(dec.at[:, others], send_sems.at[0])
    arrived(update.at[pl.ds(0, groups - EARLY_GROUPS), others], send_sems.at[1])
    arrived(early.at[:, others], send_sems.at[2])
    arrived(square_all.at[everyone], square_sems.at[0])


def write_out(*refs):
    sems = refs[-1]
    parts = len(refs) // 2
    copies = [
        pltpu.make_async_copy(refs[i], refs[parts + i], sems.at[i]) for i in range(parts)
    ]
    for copy in copies:
        copy.start()
    for copy in copies:
        copy.wait()


def shards(base_weights, inner_weights, momentum):
    replicas = lax.axis_size("replica")
    shards_count = lax.axis_size("fsdp")
    local_rows, columns = base_weights.shape
    rows = local_rows // replicas
    groups = 2 * HALF_GROUPS
    width = columns // groups
    total = float(local_rows * shards_count * columns)
    dims = (replicas, shards_count, rows, columns, groups, total)
    most = max(grid_sides(replicas))
    dma = pltpu.SemaphoreType.DMA
    blocks = (groups, replicas, rows, width)
    outside = pl.BlockSpec(memory_space=pltpu.HBM)
    vmem = pl.BlockSpec(memory_space=pltpu.VMEM)
    in_hbm = functools.partial(pltpu.with_memory_space_constraint, memory_space=pltpu.HBM)
    in_vmem = functools.partial(pltpu.with_memory_space_constraint, memory_space=pltpu.VMEM)
    held = pl.pallas_call(
        functools.partial(kernel, dims),
        out_shape=(
            pltpu.VMEM(base_weights.shape, jnp.float32),
            pltpu.VMEM(momentum.shape, jnp.float32),
            pltpu.VMEM(inner_weights.shape, jnp.bfloat16),
        ),
        in_specs=[outside] * 3,
        out_specs=(vmem, vmem, vmem),
        scratch_shapes=[
            pltpu.VMEM((local_rows, columns), jnp.float32),
            pltpu.VMEM((local_rows, columns), jnp.bfloat16),
            pltpu.VMEM((rows, columns), jnp.float32),
            pltpu.VMEM(blocks, jnp.bfloat16),
            pltpu.VMEM(blocks, jnp.bfloat16),
            pltpu.VMEM((groups, most, rows, width), jnp.bfloat16),
            pltpu.VMEM((rows, columns), jnp.float32),
            pltpu.VMEM(blocks, jnp.bfloat16),
            pltpu.VMEM((EARLY_GROUPS, replicas, 2, rows, width), jnp.bfloat16),
            pltpu.VMEM((1, BLOCK), jnp.float32),
            pltpu.VMEM((shards_count * replicas, 1, BLOCK), jnp.float32),
            dma((replicas + 2,)),
            dma((3,)),
            dma((groups, replicas - 1)),
            dma((EARLY_GROUPS, replicas - 1)),
            dma((2,)),
            pltpu.SemaphoreType.REGULAR((rounds(shards_count) + 2,)),
        ],
        compiler_params=pltpu.CompilerParams(collective_id=0, has_side_effects=True, vmem_limit_bytes=36 * 2**20),
    )(in_hbm(base_weights), in_hbm(inner_weights), in_hbm(momentum))
    return pl.pallas_call(
        write_out,
        out_shape=tuple(jax.ShapeDtypeStruct(part.shape, part.dtype) for part in held),
        in_specs=[vmem] * len(held),
        out_specs=tuple(outside for part in held),
        scratch_shapes=[dma((len(held),))],
        compiler_params=pltpu.CompilerParams(vmem_limit_bytes=2**20),
    )(*[in_vmem(part) for part in held])


def solution(mesh):
    placed = (P("fsdp", None), P("replica", "fsdp", None), P(("fsdp", "replica"), None))
    return jax.shard_map(
        shards,
        mesh=mesh,
        in_specs=placed,
        out_specs=(P("fsdp", None), P(("fsdp", "replica"), None), P("replica", "fsdp", None)),
        check_vma=False,
    )
```

```python
import functools

import jax
import jax.numpy as jnp
from jax import lax
from jax.experimental import pallas as pl
from jax.experimental.pallas import tpu as pltpu
from jax.sharding import PartitionSpec as P

BLOCK = 128
HALF_GROUPS = 4
EARLY_GROUPS = 4
EARLY_SHARE = (18, 32)
ENCODE_ROWS = 256
FIRST_GROUPS = 2
PLAIN_ROWS = 128

code_limit = 448.0
outer_rate = 0.7
outer_momentum = 0.9
blend_share = 0.5
clip_rms = 0.02
epsilon = 1e-06

MESH = pl.DeviceIdType.MESH


def decoded_deltas(deltas):
    peaks = jnp.max(jnp.abs(deltas), axis=1, keepdims=True) + epsilon
    rough = peaks * (1.0 / code_limit)
    wide = rough * (2.0**23 + 1.0)
    power = wide - (wide - rough)
    scales = jnp.where(power * code_limit < peaks, power + power, power)
    nudged = deltas * (1.0 + 2.0**-23)
    wide_deltas = nudged * (2.0**20 + 1.0)
    four_bits = wide_deltas - (wide_deltas - nudged)
    shift = scales * (1.5 * 2.0**14)
    fixed_step = (nudged + shift) - shift
    return jnp.where(jnp.abs(deltas) < scales * 2.0**-6, fixed_step, four_bits)


def arrived(blocks, sem):
    pltpu.make_async_copy(blocks, blocks, sem).wait()


def early_count(rows):
    return max(rows * EARLY_SHARE[0] // EARLY_SHARE[1] // 8 * 8, 8)


def grid_sides(replicas):
    side = 1 << (replicas.bit_length() // 2)
    while replicas % side:
        side -= 1
    return side, replicas // side


def rounds(count):
    return max(count - 2, 0).bit_length()


def kernel(
    dims,
    base_hbm, inner_hbm, momentum_hbm,
    new_base, new_momentum, new_inner,
    base_v, inner_v, momentum_v, dec, first, second, grad, update, early,
    square_mine, square_all,
    load_sems, send_sems, recv_sems, early_sems, square_sems, entry_sems,
):
    replicas, shards_count, rows, columns, groups, total = dims
    width = columns // groups
    span_x, span_y = grid_sides(replicas)
    tile = min(PLAIN_ROWS, rows)
    encode_tile = min(ENCODE_ROWS, rows)
    early_rows = early_count(rows)
    me = lax.axis_index("replica")
    row_me = lax.axis_index("fsdp")
    me_x, me_y = lax.rem(me, span_x), me // span_x

    def spans(g):
        return (span_x, span_y) if g % 2 == 0 else (span_y, span_x)

    def owner(g, dp, dq):
        dx, dy = (dp, dq) if g % 2 == 0 else (dq, dp)
        return lax.rem(me_y + dy, span_y) * span_x + lax.rem(me_x + dx, span_x)

    def near(step):
        return lax.rem(me + step, replicas)

    def far(step):
        return lax.rem(row_me + step, shards_count)

    def row_start(index):
        return pl.multiple_of(index * rows, rows)

    def greet(sem, step):
        @pl.when(row_me >= step)
        def _():
            pl.semaphore_signal(sem, inc=1, device_id={"fsdp": row_me - step}, device_id_type=MESH)

        @pl.when(row_me + step < shards_count)
        def _():
            pl.semaphore_signal(sem, inc=1, device_id={"fsdp": row_me + step}, device_id_type=MESH)

    def greeters(step):
        below = jnp.where(row_me >= step, 1, 0)
        return below + jnp.where(row_me + step < shards_count, 1, 0)

    barrier = pltpu.get_barrier_semaphore()
    beside = [owner(0, dx, 0) for dx in range(1, span_x)]
    above = [owner(0, 0, dy) for dy in range(1, span_y)]
    load_order = [(dx, dy) for dy in reversed(range(span_y)) for dx in reversed(range(span_x))]
    pieces = []
    for dx, dy in load_order:
        cuts = [0, columns] if pieces else [0, FIRST_GROUPS * width, columns]
        pieces += [((dx, dy), low, high) for low, high in zip(cuts, cuts[1:])]

    def load(at):
        (dx, dy), low, high = pieces[at]
        here = pl.ds(row_start(owner(0, dx, dy)), rows)
        cols = pl.ds(low, high - low)
        pltpu.make_async_copy(base_hbm.at[here, cols], base_v.at[here, cols], load_sems.at[at]).start()
        pltpu.make_async_copy(inner_hbm.at[0, here, cols], inner_v.at[here, cols], load_sems.at[at]).start()

    load(0)
    for peer in beside + above:
        pl.semaphore_signal(barrier, inc=1, device_id={"replica": peer}, device_id_type=MESH)

    @pl.when(row_me + 1 < shards_count)
    def _():
        pl.semaphore_signal(barrier, inc=1, device_id={"fsdp": row_me + 1}, device_id_type=MESH)

    for at in range(1, len(pieces)):
        load(at)
    momentum_load = pltpu.make_async_copy(momentum_hbm, momentum_v, load_sems.at[replicas + 1])
    momentum_load.start()

    def encode(g, dp, dq):
        slot = dp * spans(g)[1] + dq
        start = row_start(owner(g, dp, dq))

        @pl.loop(0, rows // encode_tile)
        def _(t):
            at = pl.ds(pl.multiple_of(start + t * encode_tile, encode_tile), encode_tile)
            to = pl.ds(pl.multiple_of(t * encode_tile, encode_tile), encode_tile)
            for c in range(0, width, BLOCK):
                cols = pl.ds(g * width + c, BLOCK)
                deltas = base_v[at, cols] - inner_v[at, cols].astype(jnp.float32)
                dec[g, slot, to, pl.ds(c, BLOCK)] = decoded_deltas(deltas).astype(jnp.bfloat16)

    def pair(g):
        return g // 4 * 2 + g % 2

    def copy_one(g, dp, dq):
        slot = dp * spans(g)[1] + dq
        return pltpu.make_async_remote_copy(
            src_ref=dec.at[g, slot], dst_ref=first.at[g, slot],
            send_sem=send_sems.at[0], recv_sem=recv_sems.at[pair(g), slot - 1],
            device_id={"replica": owner(g, dp, 0)}, device_id_type=MESH,
        )

    def copy_two(g, dq):
        return pltpu.make_async_remote_copy(
            src_ref=dec.at[g, dq], dst_ref=second.at[g, dq],
            send_sem=send_sems.at[0], recv_sem=recv_sems.at[pair(g), dq - 1],
            device_id={"replica": owner(g, 0, dq)}, device_id_type=MESH,
        )

    def arrival(g, dp, dq, source):
        np, nq = spans(g)
        return ((np - dp) % np) * nq + (source if dp else (nq - dq) % nq)

    def late_low(g):
        return early_rows if g < EARLY_GROUPS else 0

    def late_part(g):
        return pl.ds(late_low(g), rows - late_low(g))

    def copy_all(g, dp, dq, source):
        slot = arrival(g, dp, dq, source)
        return pltpu.make_async_remote_copy(
            src_ref=update.at[g, source if dp else 0, late_part(g)], dst_ref=update.at[g, slot, late_part(g)],
            send_sem=send_sems.at[3 if g < EARLY_GROUPS else 1], recv_sem=recv_sems.at[pair(g), slot - 1],
            device_id={"replica": owner(g, dp, dq)}, device_id_type=MESH,
        )

    def copy_early(g, dp, dq, source):
        slot = arrival(g, dp, dq, source)
        return pltpu.make_async_remote_copy(
            src_ref=early.at[g, source if dp else 0], dst_ref=early.at[g, slot],
            send_sem=send_sems.at[2], recv_sem=early_sems.at[pair(g), slot - 1],
            device_id={"replica": owner(g, dp, dq)}, device_id_type=MESH,
        )

    waited = set()

    def await_load(g, dp, dq):
        key = (dp, dq) if g % 2 == 0 else (dq, dp)
        for at, (where, low, high) in enumerate(pieces):
            if where == key and low <= g * width < high and at not in waited:
                waited.add(at)
                arrived(base_v.at[pl.ds(0, rows + rows // 2), pl.ds(0, high - low)], load_sems.at[at])

    greeted = False
    most = max(span_x, span_y)
    for dq in reversed(range(most)):
        for dp in reversed(range(1, most)):
            for g in range(groups):
                np, nq = spans(g)
                if dp < np and dq < nq:
                    await_load(g, dp, dq)
                    encode(g, dp, dq)
                    if not greeted:
                        pl.semaphore_wait(barrier, len(beside) + len(above) + jnp.where(row_me > 0, 1, 0))
                        greeted = True
                    copy_one(g, dp, dq).start()
    def sum_one(g, dq):
        np, nq = spans(g)
        if g % 4 < 2:
            for dp in range(1, np):
                slot = dp * nq + dq
                arrived(first.at[pl.ds(0, 2), slot], recv_sems.at[pair(g), slot - 1])

        @pl.loop(0, rows // tile)
        def _(t):
            at = pl.ds(pl.multiple_of(t * tile, tile), tile)
            summed = dec[g, dq, at].astype(jnp.float32)
            for dp in range(1, np):
                summed += first[g, dp * nq + dq, at].astype(jnp.float32)
            if dq:
                dec[g, dq, at] = summed.astype(jnp.bfloat16)
            else:
                grad[at, pl.ds(g * width, width)] = summed

        if dq:
            copy_two(g, dq).start()

    line_rounds = rounds(shards_count)

    def call(at):
        if at == 0:
            @pl.when(row_me > 0)
            def _():
                pl.semaphore_signal(entry_sems.at[0], inc=1, device_id={"fsdp": row_me - 1}, device_id_type=MESH)
        elif at <= line_rounds:
            greet(entry_sems.at[at], 1 << (at - 1))
        else:
            for peer in (beside, above)[at - line_rounds - 1]:
                pl.semaphore_signal(entry_sems.at[at], inc=1, device_id={"replica": peer}, device_id_type=MESH)

    def hear(at):
        if at == 0:
            @pl.when(row_me + 1 < shards_count)
            def _():
                pl.semaphore_wait(entry_sems.at[0], 1)
        elif at <= line_rounds:
            pl.semaphore_wait(entry_sems.at[at], greeters(1 << (at - 1)))
        else:
            pl.semaphore_wait(entry_sems.at[at], len((beside, above)[at - line_rounds - 1]))

    call(0)
    called = 1
    done = 0
    for dq in reversed(range(most)):
        mine = [g for g in range(groups) if dq < spans(g)[1]]
        for g in mine:
            await_load(g, 0, dq)
            encode(g, 0, dq)
            done += 1
            if done % 3 == 0 and called < line_rounds + 3:
                hear(called - 1)
                call(called)
                called += 1
        for g in mine:
            sum_one(g, dq)
    for at in range(called, line_rounds + 3):
        hear(at - 1)
        call(at)
    hear(line_rounds + 2)

    def add_group(g, squares):
        nq = spans(g)[1]
        if g % 4 < 2:
            for dq in range(1, nq):
                arrived(second.at[pl.ds(0, 2), dq], recv_sems.at[pair(g), dq - 1])

        def add(t, squares):
            at = pl.ds(pl.multiple_of(t * tile, tile), tile)
            for c in range(0, width, BLOCK):
                cols = pl.ds(g * width + c, BLOCK)
                summed = grad[at, cols]
                for dq in range(1, nq):
                    summed += second[g, dq, at, pl.ds(c, BLOCK)].astype(jnp.float32)
                outer = summed * (1.0 / replicas)
                grad[at, cols] = outer
                square = outer * outer
                for s in range(0, tile, 8):
                    squares += square[s : s + 8]
            return squares

        return lax.fori_loop(0, rows // tile, add, squares)

    def early_first(g):
        for dq in range(1, spans(g)[1]):
            copy_early(g, 0, dq, 0).start()

    def early_second(g, source):
        for dp in range(1, spans(g)[0]):
            copy_early(g, dp, 0, source).start()

    momentum_load.wait()
    for g in range(EARLY_GROUPS):
        early[g, 0, 1] = momentum_v[pl.ds(0, early_rows), pl.ds(g * width, width)].astype(jnp.bfloat16)

    squares = jnp.zeros((8, BLOCK), jnp.float32)
    for g in range(EARLY_GROUPS):
        squares = add_group(g, squares)
        early[g, 0, 0] = grad[pl.ds(0, early_rows), pl.ds(g * width, width)].astype(jnp.bfloat16)
        early_first(g)
    for g in range(EARLY_GROUPS, groups):
        squares = add_group(g, squares)

    spot = row_me * replicas + me
    square_row = jnp.sum(squares, axis=0, keepdims=True)
    square_mine[...] = square_row
    square_all[spot] = square_row
    def send_square(step, row):
        pltpu.make_async_remote_copy(
            src_ref=square_mine, dst_ref=square_all.at[spot],
            send_sem=square_sems.at[0], recv_sem=square_sems.at[1],
            device_id={"replica": near(step), "fsdp": row}, device_id_type=MESH,
        ).start()

    @pl.loop(0, shards_count - 1)
    def _(t):
        at = jnp.where(2 * row_me < shards_count, shards_count - 2 - t, t)
        row = at + jnp.where(at >= row_me, 1, 0)
        for step in reversed(range(replicas)):
            send_square(step, row)

    for step in reversed(range(1, replicas)):
        send_square(step, row_me)

    for g in range(EARLY_GROUPS):
        early_second(g, 0)
    early_sets = [(g, g + 2) for g in range(EARLY_GROUPS) if g % 4 < 2]

    def await_early(members, slot):
        arrived(early.at[pl.ds(0, 2), 0], early_sems.at[pair(members[0]), slot - 1])

    for members in early_sets:
        for dq in range(1, spans(members[0])[1]):
            await_early(members, dq)
            for g in members:
                early_second(g, dq)

    late_sets = [(g, g + 2) for g in [*range(EARLY_GROUPS, groups), *range(EARLY_GROUPS)] if g % 4 < 2]
    late = [*range(EARLY_GROUPS, groups), *range(EARLY_GROUPS)]

    def await_late(members, slot):
        arrived(update.at[pl.ds(0, 2), 0, late_part(members[0])], recv_sems.at[pair(members[0]), slot - 1])

    def pass_on(members):
        np, nq = spans(members[0])
        for dq in range(1, nq):
            await_late(members, dq)
            for g in members:
                for dp in range(1, np):
                    copy_all(g, dp, 0, dq).start()

    everyone = pl.ds(0, shards_count * replicas - 1)
    arrived(square_all.at[everyone], square_sems.at[1])
    squares = jnp.sum(square_all[...], axis=0)
    mean_square = jnp.broadcast_to(jnp.sum(squares, axis=1, keepdims=True), (1, BLOCK)) / total
    clip_factor = jnp.minimum(1.0, clip_rms / jnp.sqrt(mean_square + epsilon))

    def moved_and_change(outer, kept):
        step_term = clip_factor * outer
        moved = outer_momentum * kept + step_term
        return moved, step_term + outer_momentum * moved

    def advance(g, low, high, sends):
        for at in range(low, high, tile):
            part = pl.ds(at, min(tile, high - at))
            for c in range(0, width, BLOCK):
                cols = pl.ds(g * width + c, BLOCK)
                moved, change = moved_and_change(grad[part, cols], momentum_v[part, cols])
                new_momentum[part, cols] = moved
                if sends:
                    update[g, 0, part, pl.ds(c, BLOCK)] = change.astype(jnp.bfloat16)

    for g in late:
        advance(g, late_low(g), rows, True)
        for dq in range(1, spans(g)[1]):
            copy_all(g, 0, dq, 0).start()
    for g in late:
        for dp in range(1, spans(g)[0]):
            copy_all(g, dp, 0, 0).start()

    def finish(g, slot, start, low, high, change_at):
        def block(part_low, size):
            at = pl.ds(pl.multiple_of(start + part_low, 8), size)
            to = pl.ds(part_low, size)
            for c in range(0, width, BLOCK):
                cols = pl.ds(g * width + c, BLOCK)
                change = change_at(g, slot, to, pl.ds(c, BLOCK))
                fresh = base_v[at, cols] - outer_rate * change
                new_base[at, cols] = fresh
                blended = blend_share * inner_v[at, cols].astype(jnp.float32) + (
                    1.0 - blend_share
                ) * fresh
                new_inner[0, at, cols] = blended.astype(jnp.bfloat16)

        for at in range(low, high, tile):
            block(at, min(tile, high - at))

    def early_change(g, slot, to, cols):
        _, change = moved_and_change(
            early[g, slot, 0, to, cols].astype(jnp.float32),
            early[g, slot, 1, to, cols].astype(jnp.float32),
        )
        return change

    def late_change(g, slot, to, cols):
        return update[g, slot, to, cols].astype(jnp.float32)

    def finish_early(g, dp, dq):
        slot = dp * spans(g)[1] + dq
        finish(g, slot, row_start(owner(g, dp, dq)), 0, early_rows, early_change)

    def finish_late(g, dp, dq):
        slot = dp * spans(g)[1] + dq
        finish(g, slot, row_start(owner(g, dp, dq)), late_low(g), rows, late_change)

    for g in range(EARLY_GROUPS):
        advance(g, 0, early_rows, False)
        for dq in range(spans(g)[1]):
            finish_early(g, 0, dq)
    for g in late:
        finish_late(g, 0, 0)
    for members in late_sets:
        pass_on(members)
    for g in late:
        for dq in range(1, spans(g)[1]):
            finish_late(g, 0, dq)
    for dq in range(most):
        for members in early_sets:
            np, nq = spans(members[0])
            for dp in range(1, np if dq < nq else 1):
                await_early(members, dp * nq + dq)
                for g in members:
                    finish_early(g, dp, dq)
        for members in late_sets:
            np, nq = spans(members[0])
            for dp in range(1, np if dq < nq else 1):
                await_late(members, dp * nq + dq)
                for g in members:
                    finish_late(g, dp, dq)
    others = pl.ds(0, replicas - 1)
    arrived(dec.at[:, others], send_sems.at[0])
    arrived(update.at[pl.ds(0, groups - EARLY_GROUPS), others], send_sems.at[1])
    arrived(update.at[pl.ds(0, EARLY_GROUPS), others, late_part(0)], send_sems.at[3])
    arrived(early.at[:, others], send_sems.at[2])
    arrived(square_all.at[everyone], square_sems.at[0])


def write_out(*refs):
    sems = refs[-1]
    parts = len(refs) // 2
    copies = [
        pltpu.make_async_copy(refs[i], refs[parts + i], sems.at[i]) for i in range(parts)
    ]
    for copy in copies:
        copy.start()
    for copy in copies:
        copy.wait()


def shards(base_weights, inner_weights, momentum):
    replicas = lax.axis_size("replica")
    shards_count = lax.axis_size("fsdp")
    local_rows, columns = base_weights.shape
    rows = local_rows // replicas
    groups = 2 * HALF_GROUPS
    width = columns // groups
    total = float(local_rows * shards_count * columns)
    dims = (replicas, shards_count, rows, columns, groups, total)
    most = max(grid_sides(replicas))
    dma = pltpu.SemaphoreType.DMA
    blocks = (groups, replicas, rows, width)
    outside = pl.BlockSpec(memory_space=pltpu.HBM)
    vmem = pl.BlockSpec(memory_space=pltpu.VMEM)
    in_hbm = functools.partial(pltpu.with_memory_space_constraint, memory_space=pltpu.HBM)
    in_vmem = functools.partial(pltpu.with_memory_space_constraint, memory_space=pltpu.VMEM)
    held = pl.pallas_call(
        functools.partial(kernel, dims),
        out_shape=(
            pltpu.VMEM(base_weights.shape, jnp.float32),
            pltpu.VMEM(momentum.shape, jnp.float32),
            pltpu.VMEM(inner_weights.shape, jnp.bfloat16),
        ),
        in_specs=[outside] * 3,
        out_specs=(vmem, vmem, vmem),
        scratch_shapes=[
            pltpu.VMEM((local_rows, columns), jnp.float32),
            pltpu.VMEM((local_rows, columns), jnp.bfloat16),
            pltpu.VMEM((rows, columns), jnp.float32),
            pltpu.VMEM(blocks, jnp.bfloat16),
            pltpu.VMEM(blocks, jnp.bfloat16),
            pltpu.VMEM((groups, most, rows, width), jnp.bfloat16),
            pltpu.VMEM((rows, columns), jnp.float32),
            pltpu.VMEM(blocks, jnp.bfloat16),
            pltpu.VMEM((EARLY_GROUPS, replicas, 2, early_count(rows), width), jnp.bfloat16),
            pltpu.VMEM((1, BLOCK), jnp.float32),
            pltpu.VMEM((shards_count * replicas, 1, BLOCK), jnp.float32),
            dma((replicas + 2,)),
            dma((4,)),
            dma((groups // 2, replicas - 1)),
            dma((EARLY_GROUPS // 2, replicas - 1)),
            dma((2,)),
            pltpu.SemaphoreType.REGULAR((rounds(shards_count) + 3,)),
        ],
        compiler_params=pltpu.CompilerParams(collective_id=0, has_side_effects=True, vmem_limit_bytes=36 * 2**20),
    )(in_hbm(base_weights), in_hbm(inner_weights), in_hbm(momentum))
    return pl.pallas_call(
        write_out,
        out_shape=tuple(jax.ShapeDtypeStruct(part.shape, part.dtype) for part in held),
        in_specs=[vmem] * len(held),
        out_specs=tuple(outside for part in held),
        scratch_shapes=[dma((len(held),))],
        compiler_params=pltpu.CompilerParams(vmem_limit_bytes=2**20),
    )(*[in_vmem(part) for part in held])


def solution(mesh):
    placed = (P("fsdp", None), P("replica", "fsdp", None), P(("fsdp", "replica"), None))
    return jax.shard_map(
        shards,
        mesh=mesh,
        in_specs=placed,
        out_specs=(P("fsdp", None), P(("fsdp", "replica"), None), P("replica", "fsdp", None)),
        check_vma=False,
    )
```

```python
import functools

import jax
import jax.numpy as jnp
from jax import lax
from jax.experimental import pallas as pl
from jax.experimental.pallas import tpu as pltpu
from jax.sharding import PartitionSpec as P

BLOCK = 128
HALF_GROUPS = 4
EARLY_GROUPS = 4
EARLY_SHARE = (18, 32)
ENCODE_ROWS = 256
FIRST_GROUPS = 2
PLAIN_ROWS = 128

code_limit = 448.0
outer_rate = 0.7
outer_momentum = 0.9
blend_share = 0.5
clip_rms = 0.02
epsilon = 1e-06

MESH = pl.DeviceIdType.MESH


def decoded_deltas(deltas):
    peaks = jnp.max(jnp.abs(deltas), axis=1, keepdims=True) + epsilon
    rough = peaks * (1.0 / code_limit)
    wide = rough * (2.0**23 + 1.0)
    power = wide - (wide - rough)
    scales = jnp.where(power * code_limit < peaks, power + power, power)
    nudged = deltas * (1.0 + 2.0**-23)
    wide_deltas = nudged * (2.0**20 + 1.0)
    four_bits = wide_deltas - (wide_deltas - nudged)
    shift = scales * (1.5 * 2.0**14)
    fixed_step = (nudged + shift) - shift
    return jnp.where(jnp.abs(deltas) < scales * 2.0**-6, fixed_step, four_bits)


def arrived(blocks, sem):
    pltpu.make_async_copy(blocks, blocks, sem).wait()


def early_count(rows):
    return max(rows * EARLY_SHARE[0] // EARLY_SHARE[1] // 8 * 8, 8)


def grid_sides(replicas):
    side = 1 << (replicas.bit_length() // 2)
    while replicas % side:
        side -= 1
    return side, replicas // side


def rounds(count):
    return max(count - 2, 0).bit_length()


def kernel(
    dims,
    base_hbm, inner_hbm, momentum_hbm,
    new_base, new_momentum, new_inner,
    base_v, inner_v, momentum_v, dec, first, second, grad, update, early,
    square_mine, square_all,
    load_sems, send_sems, recv_sems, early_sems, square_sems, entry_sems,
):
    replicas, shards_count, rows, columns, groups, total = dims
    width = columns // groups
    span_x, span_y = grid_sides(replicas)
    tile = min(PLAIN_ROWS, rows)
    encode_tile = min(ENCODE_ROWS, rows)
    early_rows = early_count(rows)
    me = lax.axis_index("replica")
    row_me = lax.axis_index("fsdp")
    me_x, me_y = lax.rem(me, span_x), me // span_x

    def spans(g):
        return (span_x, span_y) if g % 2 == 0 else (span_y, span_x)

    def owner(g, dp, dq):
        dx, dy = (dp, dq) if g % 2 == 0 else (dq, dp)
        return lax.rem(me_y + dy, span_y) * span_x + lax.rem(me_x + dx, span_x)

    def near(step):
        return lax.rem(me + step, replicas)

    def far(step):
        return lax.rem(row_me + step, shards_count)

    def row_start(index):
        return pl.multiple_of(index * rows, rows)

    def greet(sem, step):
        @pl.when(row_me >= step)
        def _():
            pl.semaphore_signal(sem, inc=1, device_id={"fsdp": row_me - step}, device_id_type=MESH)

        @pl.when(row_me + step < shards_count)
        def _():
            pl.semaphore_signal(sem, inc=1, device_id={"fsdp": row_me + step}, device_id_type=MESH)

    def greeters(step):
        below = jnp.where(row_me >= step, 1, 0)
        return below + jnp.where(row_me + step < shards_count, 1, 0)

    barrier = pltpu.get_barrier_semaphore()
    beside = [owner(0, dx, 0) for dx in range(1, span_x)]
    above = [owner(0, 0, dy) for dy in range(1, span_y)]
    load_order = [(dx, dy) for dy in reversed(range(span_y)) for dx in reversed(range(span_x))]
    pieces = []
    for dx, dy in load_order:
        cuts = [0, columns] if pieces else [0, FIRST_GROUPS * width, columns]
        pieces += [((dx, dy), low, high) for low, high in zip(cuts, cuts[1:])]

    def load(at):
        (dx, dy), low, high = pieces[at]
        here = pl.ds(row_start(owner(0, dx, dy)), rows)
        cols = pl.ds(low, high - low)
        pltpu.make_async_copy(base_hbm.at[here, cols], base_v.at[here, cols], load_sems.at[at]).start()
        pltpu.make_async_copy(inner_hbm.at[0, here, cols], inner_v.at[here, cols], load_sems.at[at]).start()

    load(0)
    for peer in beside + above:
        pl.semaphore_signal(barrier, inc=1, device_id={"replica": peer}, device_id_type=MESH)

    @pl.when(row_me + 1 < shards_count)
    def _():
        pl.semaphore_signal(barrier, inc=1, device_id={"fsdp": row_me + 1}, device_id_type=MESH)

    for at in range(1, len(pieces)):
        load(at)
    momentum_load = pltpu.make_async_copy(momentum_hbm, momentum_v, load_sems.at[replicas + 1])
    momentum_load.start()

    def encode(g, dp, dq):
        slot = dp * spans(g)[1] + dq
        start = row_start(owner(g, dp, dq))

        @pl.loop(0, rows // encode_tile)
        def _(t):
            at = pl.ds(pl.multiple_of(start + t * encode_tile, encode_tile), encode_tile)
            to = pl.ds(pl.multiple_of(t * encode_tile, encode_tile), encode_tile)
            for c in range(0, width, BLOCK):
                cols = pl.ds(g * width + c, BLOCK)
                deltas = base_v[at, cols] - inner_v[at, cols].astype(jnp.float32)
                dec[g, slot, to, pl.ds(c, BLOCK)] = decoded_deltas(deltas).astype(jnp.bfloat16)

    def pair(g):
        return g // 4 * 2 + g % 2

    def copy_one(g, dp, dq):
        slot = dp * spans(g)[1] + dq
        return pltpu.make_async_remote_copy(
            src_ref=dec.at[g, slot], dst_ref=first.at[g, slot],
            send_sem=send_sems.at[0], recv_sem=recv_sems.at[pair(g), slot - 1],
            device_id={"replica": owner(g, dp, 0)}, device_id_type=MESH,
        )

    def copy_two(g, dq):
        return pltpu.make_async_remote_copy(
            src_ref=dec.at[g, dq], dst_ref=second.at[g, dq],
            send_sem=send_sems.at[0], recv_sem=recv_sems.at[pair(g), dq - 1],
            device_id={"replica": owner(g, 0, dq)}, device_id_type=MESH,
        )

    def arrival(g, dp, dq, source):
        np, nq = spans(g)
        return ((np - dp) % np) * nq + (source if dp else (nq - dq) % nq)

    def late_low(g):
        return early_rows if g < EARLY_GROUPS else 0

    def late_part(g):
        return pl.ds(late_low(g), rows - late_low(g))

    def copy_all(g, dp, dq, source):
        slot = arrival(g, dp, dq, source)
        return pltpu.make_async_remote_copy(
            src_ref=update.at[g, source if dp else 0, late_part(g)], dst_ref=update.at[g, slot, late_part(g)],
            send_sem=send_sems.at[3 if g < EARLY_GROUPS else 1], recv_sem=recv_sems.at[pair(g), slot - 1],
            device_id={"replica": owner(g, dp, dq)}, device_id_type=MESH,
        )

    def copy_early(g, dp, dq, source):
        slot = arrival(g, dp, dq, source)
        return pltpu.make_async_remote_copy(
            src_ref=early.at[g, source if dp else 0], dst_ref=early.at[g, slot],
            send_sem=send_sems.at[2], recv_sem=early_sems.at[pair(g), slot - 1],
            device_id={"replica": owner(g, dp, dq)}, device_id_type=MESH,
        )

    waited = set()

    def await_load(g, dp, dq):
        key = (dp, dq) if g % 2 == 0 else (dq, dp)
        for at, (where, low, high) in enumerate(pieces):
            if where == key and low <= g * width < high and at not in waited:
                waited.add(at)
                arrived(base_v.at[pl.ds(0, rows + rows // 2), pl.ds(0, high - low)], load_sems.at[at])

    greeted = False
    most = max(span_x, span_y)
    for dq in reversed(range(most)):
        for dp in reversed(range(1, most)):
            for g in range(groups):
                np, nq = spans(g)
                if dp < np and dq < nq:
                    await_load(g, dp, dq)
                    encode(g, dp, dq)
                    if not greeted:
                        pl.semaphore_wait(barrier, len(beside) + len(above) + jnp.where(row_me > 0, 1, 0))
                        greeted = True
                    copy_one(g, dp, dq).start()
    def sum_one(g, dq):
        np, nq = spans(g)
        if g % 4 < 2:
            for dp in range(1, np):
                slot = dp * nq + dq
                arrived(first.at[pl.ds(0, 2), slot], recv_sems.at[pair(g), slot - 1])

        if not dq:
            return

        @pl.loop(0, rows // tile)
        def _(t):
            at = pl.ds(pl.multiple_of(t * tile, tile), tile)
            summed = dec[g, dq, at].astype(jnp.float32)
            for dp in range(1, np):
                summed += first[g, dp * nq + dq, at].astype(jnp.float32)
            dec[g, dq, at] = summed.astype(jnp.bfloat16)

        copy_two(g, dq).start()

    line_rounds = rounds(shards_count)

    def call(at):
        if at == 0:
            @pl.when(row_me > 0)
            def _():
                pl.semaphore_signal(entry_sems.at[0], inc=1, device_id={"fsdp": row_me - 1}, device_id_type=MESH)
        elif at <= line_rounds:
            greet(entry_sems.at[at], 1 << (at - 1))
        else:
            for peer in (beside, above)[at - line_rounds - 1]:
                pl.semaphore_signal(entry_sems.at[at], inc=1, device_id={"replica": peer}, device_id_type=MESH)

    def hear(at):
        if at == 0:
            @pl.when(row_me + 1 < shards_count)
            def _():
                pl.semaphore_wait(entry_sems.at[0], 1)
        elif at <= line_rounds:
            pl.semaphore_wait(entry_sems.at[at], greeters(1 << (at - 1)))
        else:
            pl.semaphore_wait(entry_sems.at[at], len((beside, above)[at - line_rounds - 1]))

    call(0)
    called = 1
    done = 0
    for dq in reversed(range(most)):
        mine = [g for g in range(groups) if dq < spans(g)[1]]
        for g in mine:
            await_load(g, 0, dq)
            encode(g, 0, dq)
            done += 1
            if done % 3 == 0 and called < line_rounds + 3:
                hear(called - 1)
                call(called)
                called += 1
        for g in mine:
            sum_one(g, dq)
    for at in range(called, line_rounds + 3):
        hear(at - 1)
        call(at)
    hear(line_rounds + 2)

    def add_group(g, squares):
        np, nq = spans(g)
        if g % 4 < 2:
            for dq in range(1, nq):
                arrived(second.at[pl.ds(0, 2), dq], recv_sems.at[pair(g), dq - 1])

        def add(t, squares):
            at = pl.ds(pl.multiple_of(t * tile, tile), tile)
            for c in range(0, width, BLOCK):
                cols = pl.ds(g * width + c, BLOCK)
                summed = dec[g, 0, at, pl.ds(c, BLOCK)].astype(jnp.float32)
                for dp in range(1, np):
                    summed += first[g, dp * nq, at, pl.ds(c, BLOCK)].astype(jnp.float32)
                for dq in range(1, nq):
                    summed += second[g, dq, at, pl.ds(c, BLOCK)].astype(jnp.float32)
                outer = summed * (1.0 / replicas)
                grad[at, cols] = outer
                square = outer * outer
                for s in range(0, tile, 8):
                    squares += square[s : s + 8]
            return squares

        return lax.fori_loop(0, rows // tile, add, squares)

    def early_first(g):
        for dq in range(1, spans(g)[1]):
            copy_early(g, 0, dq, 0).start()

    def early_second(g, source):
        for dp in range(1, spans(g)[0]):
            copy_early(g, dp, 0, source).start()

    momentum_load.wait()
    for g in range(EARLY_GROUPS):
        early[g, 0, 1] = momentum_v[pl.ds(0, early_rows), pl.ds(g * width, width)].astype(jnp.bfloat16)

    squares = jnp.zeros((8, BLOCK), jnp.float32)
    for g in range(EARLY_GROUPS):
        squares = add_group(g, squares)
        early[g, 0, 0] = grad[pl.ds(0, early_rows), pl.ds(g * width, width)].astype(jnp.bfloat16)
        early_first(g)
    for g in range(EARLY_GROUPS, groups):
        squares = add_group(g, squares)

    spot = row_me * replicas + me
    square_row = jnp.sum(squares, axis=0, keepdims=True)
    square_mine[...] = square_row
    square_all[spot] = square_row
    def send_square(step, row):
        pltpu.make_async_remote_copy(
            src_ref=square_mine, dst_ref=square_all.at[spot],
            send_sem=square_sems.at[0], recv_sem=square_sems.at[1],
            device_id={"replica": near(step), "fsdp": row}, device_id_type=MESH,
        ).start()

    @pl.loop(0, shards_count - 1)
    def _(t):
        at = jnp.where(2 * row_me < shards_count, shards_count - 2 - t, t)
        row = at + jnp.where(at >= row_me, 1, 0)
        for step in reversed(range(replicas)):
            send_square(step, row)

    for step in reversed(range(1, replicas)):
        send_square(step, row_me)

    for g in range(EARLY_GROUPS):
        early_second(g, 0)
    early_sets = [(g, g + 2) for g in range(EARLY_GROUPS) if g % 4 < 2]

    def await_early(members, slot):
        arrived(early.at[pl.ds(0, 2), 0], early_sems.at[pair(members[0]), slot - 1])

    for members in early_sets:
        for dq in range(1, spans(members[0])[1]):
            await_early(members, dq)
            for g in members:
                early_second(g, dq)

    late_sets = [(g, g + 2) for g in [*range(EARLY_GROUPS, groups), *range(EARLY_GROUPS)] if g % 4 < 2]
    late = [*range(EARLY_GROUPS, groups), *range(EARLY_GROUPS)]

    def await_late(members, slot):
        arrived(update.at[pl.ds(0, 2), 0, late_part(members[0])], recv_sems.at[pair(members[0]), slot - 1])

    def pass_on(members):
        np, nq = spans(members[0])
        for dq in range(1, nq):
            await_late(members, dq)
            for g in members:
                for dp in range(1, np):
                    copy_all(g, dp, 0, dq).start()

    everyone = pl.ds(0, shards_count * replicas - 1)
    arrived(square_all.at[everyone], square_sems.at[1])
    squares = jnp.sum(square_all[...], axis=0)
    mean_square = jnp.broadcast_to(jnp.sum(squares, axis=1, keepdims=True), (1, BLOCK)) / total
    clip_factor = jnp.minimum(1.0, clip_rms / jnp.sqrt(mean_square + epsilon))

    def moved_and_change(outer, kept):
        step_term = clip_factor * outer
        moved = outer_momentum * kept + step_term
        return moved, step_term + outer_momentum * moved

    def advance(g, low, high, sends):
        for at in range(low, high, tile):
            part = pl.ds(at, min(tile, high - at))
            for c in range(0, width, BLOCK):
                cols = pl.ds(g * width + c, BLOCK)
                moved, change = moved_and_change(grad[part, cols], momentum_v[part, cols])
                if sends:
                    update[g, 0, part, pl.ds(c, BLOCK)] = change.astype(jnp.bfloat16)
                else:
                    new_momentum[part, cols] = moved

    for g in late:
        advance(g, late_low(g), rows, True)
        for dq in range(1, spans(g)[1]):
            copy_all(g, 0, dq, 0).start()
    for g in late:
        for dp in range(1, spans(g)[0]):
            copy_all(g, dp, 0, 0).start()

    def finish(g, slot, start, low, high, change_at):
        def block(part_low, size):
            at = pl.ds(pl.multiple_of(start + part_low, 8), size)
            to = pl.ds(part_low, size)
            for c in range(0, width, BLOCK):
                cols = pl.ds(g * width + c, BLOCK)
                change = change_at(g, slot, to, pl.ds(c, BLOCK))
                fresh = base_v[at, cols] - outer_rate * change
                new_base[at, cols] = fresh
                blended = blend_share * inner_v[at, cols].astype(jnp.float32) + (
                    1.0 - blend_share
                ) * fresh
                new_inner[0, at, cols] = blended.astype(jnp.bfloat16)

        for at in range(low, high, tile):
            block(at, min(tile, high - at))

    def early_change(g, slot, to, cols):
        _, change = moved_and_change(
            early[g, slot, 0, to, cols].astype(jnp.float32),
            early[g, slot, 1, to, cols].astype(jnp.float32),
        )
        return change

    def late_change(g, slot, to, cols):
        return update[g, slot, to, cols].astype(jnp.float32)

    def finish_early(g, dp, dq):
        slot = dp * spans(g)[1] + dq
        finish(g, slot, row_start(owner(g, dp, dq)), 0, early_rows, early_change)

    def finish_late(g, dp, dq):
        slot = dp * spans(g)[1] + dq
        finish(g, slot, row_start(owner(g, dp, dq)), late_low(g), rows, late_change)

    for g in range(EARLY_GROUPS):
        for dq in range(spans(g)[1]):
            finish_early(g, 0, dq)
    for g in late:
        finish_late(g, 0, 0)
        advance(g, 0, rows, False)
    for members in late_sets:
        pass_on(members)
    for g in late:
        for dq in range(1, spans(g)[1]):
            finish_late(g, 0, dq)
    for dq in range(most):
        for members in early_sets:
            np, nq = spans(members[0])
            for dp in range(1, np if dq < nq else 1):
                await_early(members, dp * nq + dq)
                for g in members:
                    finish_early(g, dp, dq)
        for members in late_sets:
            np, nq = spans(members[0])
            for dp in range(1, np if dq < nq else 1):
                await_late(members, dp * nq + dq)
                for g in members:
                    finish_late(g, dp, dq)
    others = pl.ds(0, replicas - 1)
    arrived(dec.at[:, others], send_sems.at[0])
    arrived(update.at[pl.ds(0, groups - EARLY_GROUPS), others], send_sems.at[1])
    arrived(update.at[pl.ds(0, EARLY_GROUPS), others, late_part(0)], send_sems.at[3])
    arrived(early.at[:, others], send_sems.at[2])
    arrived(square_all.at[everyone], square_sems.at[0])


def write_out(*refs):
    sems = refs[-1]
    parts = len(refs) // 2
    copies = [
        pltpu.make_async_copy(refs[i], refs[parts + i], sems.at[i]) for i in range(parts)
    ]
    for copy in copies:
        copy.start()
    for copy in copies:
        copy.wait()


def shards(base_weights, inner_weights, momentum):
    replicas = lax.axis_size("replica")
    shards_count = lax.axis_size("fsdp")
    local_rows, columns = base_weights.shape
    rows = local_rows // replicas
    groups = 2 * HALF_GROUPS
    width = columns // groups
    total = float(local_rows * shards_count * columns)
    dims = (replicas, shards_count, rows, columns, groups, total)
    most = max(grid_sides(replicas))
    dma = pltpu.SemaphoreType.DMA
    blocks = (groups, replicas, rows, width)
    outside = pl.BlockSpec(memory_space=pltpu.HBM)
    vmem = pl.BlockSpec(memory_space=pltpu.VMEM)
    in_hbm = functools.partial(pltpu.with_memory_space_constraint, memory_space=pltpu.HBM)
    in_vmem = functools.partial(pltpu.with_memory_space_constraint, memory_space=pltpu.VMEM)
    held = pl.pallas_call(
        functools.partial(kernel, dims),
        out_shape=(
            pltpu.VMEM(base_weights.shape, jnp.float32),
            pltpu.VMEM(momentum.shape, jnp.float32),
            pltpu.VMEM(inner_weights.shape, jnp.bfloat16),
        ),
        in_specs=[outside] * 3,
        out_specs=(vmem, vmem, vmem),
        scratch_shapes=[
            pltpu.VMEM((local_rows, columns), jnp.float32),
            pltpu.VMEM((local_rows, columns), jnp.bfloat16),
            pltpu.VMEM((rows, columns), jnp.float32),
            pltpu.VMEM(blocks, jnp.bfloat16),
            pltpu.VMEM(blocks, jnp.bfloat16),
            pltpu.VMEM((groups, most, rows, width), jnp.bfloat16),
            pltpu.VMEM((rows, columns), jnp.float32),
            pltpu.VMEM(blocks, jnp.bfloat16),
            pltpu.VMEM((EARLY_GROUPS, replicas, 2, early_count(rows), width), jnp.bfloat16),
            pltpu.VMEM((1, BLOCK), jnp.float32),
            pltpu.VMEM((shards_count * replicas, 1, BLOCK), jnp.float32),
            dma((replicas + 2,)),
            dma((4,)),
            dma((groups // 2, replicas - 1)),
            dma((EARLY_GROUPS // 2, replicas - 1)),
            dma((2,)),
            pltpu.SemaphoreType.REGULAR((rounds(shards_count) + 3,)),
        ],
        compiler_params=pltpu.CompilerParams(collective_id=0, has_side_effects=True, vmem_limit_bytes=36 * 2**20),
    )(in_hbm(base_weights), in_hbm(inner_weights), in_hbm(momentum))
    return pl.pallas_call(
        write_out,
        out_shape=tuple(jax.ShapeDtypeStruct(part.shape, part.dtype) for part in held),
        in_specs=[vmem] * len(held),
        out_specs=tuple(outside for part in held),
        scratch_shapes=[dma((len(held),))],
        compiler_params=pltpu.CompilerParams(vmem_limit_bytes=2**20),
    )(*[in_vmem(part) for part in held])


def solution(mesh):
    placed = (P("fsdp", None), P("replica", "fsdp", None), P(("fsdp", "replica"), None))
    return jax.shard_map(
        shards,
        mesh=mesh,
        in_specs=placed,
        out_specs=(P("fsdp", None), P(("fsdp", "replica"), None), P("replica", "fsdp", None)),
        check_vma=False,
    )
```
